32 devices in a mesh: ctx: 16 (over z, y, core), fsdp: 2 (over x).
Axes of the slice: x: 2, y: 2, z: 4, core: 2. Of those that a mesh axis runs over, the one named last changes fastest.
Arguments:
- block_input: bfloat16 [2, 16, 128, 1024], P(None, 'ctx', 'fsdp'), may hold values from -6 to 6
- dy: bfloat16 [2, 16, 128, 1024], P(None, 'ctx', 'fsdp'), may hold values from -6 to 6
- attn_gain: float32 [1024], replicated, may hold values from 0.25 to 1.75
- q_gain: float32 [64], replicated, may hold values from 0.7 to 1.4, as said below
- k_gain: float32 [64], replicated, may hold values from 0.7 to 1.4, as said below
- ffn_gain: float32 [1024], replicated, may hold values from 0.25 to 1.75
- wq: bfloat16 [1024, 1024], P('fsdp'), may hold values from -0.1875 to 0.1875
- wk: bfloat16 [1024, 512], P('fsdp'), may hold values from -0.1875 to 0.1875
- wv: bfloat16 [1024, 512], P('fsdp'), may hold values from -0.1875 to 0.1875
- wo: bfloat16 [1024, 1024], P('fsdp'), may hold values from -1.5 to 1.5
- w_gate: bfloat16 [1024, 4608], P('fsdp'), may hold values from -0.1875 to 0.1875
- w_up: bfloat16 [1024, 4608], P('fsdp'), may hold values from -0.1875 to 0.1875
- w_down: bfloat16 [4608, 1024], P('fsdp'), may hold values from -0.09375 to 0.09375
Outputs:
- block_output: bfloat16 [2, 16, 128, 1024], P(None, 'ctx', 'fsdp')
- dx: float32 [2, 16, 128, 1024], P(None, 'ctx', 'fsdp')
- d_attn_gain: float32 [1024], replicated
- d_q_gain: float32 [64], replicated
- d_k_gain: float32 [64], replicated
- d_ffn_gain: float32 [1024], replicated
- d_wq: float32 [1024, 1024], P(('ctx', 'fsdp'))
- d_wk: float32 [1024, 512], P(('ctx', 'fsdp'))
- d_wv: float32 [1024, 512], P(('ctx', 'fsdp'))
- d_wo: float32 [1024, 1024], P(('ctx', 'fsdp'))
- d_w_gate: float32 [1024, 4608], P(('ctx', 'fsdp'))
- d_w_up: float32 [1024, 4608], P(('ctx', 'fsdp'))
- d_w_down: float32 [4608, 1024], P(('ctx', 'fsdp'))
The draws below stay inside these ranges and needn't reach their ends.
Inputs may be any that keep to these rules, and one draw needn't show every extreme that they name: `q_gain`: each entry is a positive gain. `k_gain`: each entry is a positive gain.
All inputs are finite; a program needn't handle non-finite values.
Results may differ from the reference program's by a relative error of at most 0.014.
Values may be sent and summed in bfloat16 or wider, within the bound.
A program may use at most 448 MiB of HBM per device.

```python
import math
import jax
import jax.numpy as jnp
from jax import lax

D = 1024
FF = 4608
QUERY_HEADS = 16
KEY_VALUE_HEADS = 8
HEAD_SIZE = 64
BLK = 128
PAIRS = 16
QW = 1024
KVW = 512


def head_gain(key, salt):
    lower, upper = (0.7, 1.4)
    uniform_draw = jax.random.uniform(jax.random.fold_in(key, salt), (HEAD_SIZE,), jnp.float32)
    return jnp.exp(jnp.log(lower) + uniform_draw * (jnp.log(upper) - jnp.log(lower)))


def draw_q_gain(key, part):
    return head_gain(key, 11)


def draw_k_gain(key, part):
    return head_gain(key, 23)


def shard_levels(key, shape, pieces, smallest, high):
    def one(position, blocks):
        heights = jax.random.uniform(jax.random.fold_in(jax.random.fold_in(key, 6), position), (blocks,), jnp.float32, smallest / len(pieces), high / len(pieces))
        return jnp.repeat(jnp.exp(heights), shape[position] // blocks).reshape((-1,) + (1,) * (len(shape) - position - 1))

    factor_of = one(*pieces[0])
    for cut in pieces[1:]:
        factor_of = factor_of * one(*cut)
    return factor_of


def scatter_about(stream_key, dims, spread, reach, split=(), kind=jnp.bfloat16):
    factor_of = shard_levels(stream_key, dims, split, -0.22, 0.18) if split else 1.0
    entries = jax.random.normal(stream_key, dims, jnp.float32) * spread * factor_of
    return jnp.minimum(jnp.maximum(entries, -reach), reach).astype(kind)


def setup_inputs(seed: int = 0) -> dict:
    keys = jax.random.split(jax.random.key(seed), 14)
    block_input = scatter_about(keys[0], (2, PAIRS, BLK, D), 1.0, 6.0, ((1, 16), (2, 2)))
    dy = scatter_about(keys[1], (2, PAIRS, BLK, D), 1.0, 6.0, ((1, 16), (2, 2)))
    attn_gain = jnp.clip(1.0 + 0.15 * jax.random.normal(keys[2], (D,), jnp.float32), 0.25, 1.75)
    q_gain = draw_q_gain(jax.random.fold_in(keys[13], 71), 0)
    k_gain = draw_k_gain(jax.random.fold_in(keys[13], 71), 0)
    ffn_gain = jnp.clip(1.0 + 0.15 * jax.random.normal(keys[5], (D,), jnp.float32), 0.25, 1.75)
    wq = scatter_about(keys[6], (D, QW), D ** -0.5, 0.1875, ((0, 2),))
    wk = scatter_about(keys[7], (D, KVW), D ** -0.5, 0.1875, ((0, 2),))
    wv = scatter_about(keys[8], (D, KVW), D ** -0.5, 0.1875, ((0, 2),))
    wo = scatter_about(keys[9], (QW, D), 16 ** -0.5, 1.5, ((0, 2),))
    w_gate = scatter_about(keys[10], (D, FF), D ** -0.5, 0.1875, ((0, 2),))
    w_up = scatter_about(keys[11], (D, FF), D ** -0.5, 0.1875, ((0, 2),))
    w_down = scatter_about(keys[12], (FF, D), FF ** -0.5, 0.09375, ((0, 2),))
    return {"block_input": block_input, "dy": dy, "attn_gain": attn_gain, "q_gain": q_gain, "k_gain": k_gain, "ffn_gain": ffn_gain, "wq": wq, "wk": wk, "wv": wv, "wo": wo, "w_gate": w_gate, "w_up": w_up, "w_down": w_down}


EPS = 1e-05
ROPE_BASE = 1000000.0

def rms_forward(inputs, gain_vec):
    inverse = lax.rsqrt(lax.optimization_barrier(jnp.mean(inputs * inputs, axis=-1, keepdims=True)) + EPS)
    return (inputs * inverse * gain_vec, inverse)

def rms_backward(inputs, inverse, gain_vec, grad_out):
    scaled = grad_out * gain_vec
    inner_mean = lax.optimization_barrier(jnp.mean(scaled * inputs, axis=-1, keepdims=True))
    grad_in = inverse * scaled - inputs * (inverse * inverse * inverse) * inner_mean
    grad_gain = lax.optimization_barrier(jnp.sum((grad_out * inputs * inverse).reshape(-1, inputs.shape[-1]), axis=0))
    return (grad_in, grad_gain)

def rope_tables(positions, head_width):
    frequency = ROPE_BASE ** (-2.0 * jnp.arange(head_width // 2, dtype=jnp.float32) / head_width)
    angles = positions.astype(jnp.float32)[:, None] * frequency[None, :]
    cosine = jnp.concatenate([jnp.cos(angles), jnp.cos(angles)], axis=-1)[:, None, :]
    sine_tab = jnp.concatenate([jnp.sin(angles), jnp.sin(angles)], axis=-1)[:, None, :]
    return (cosine, sine_tab)

def rotate(inputs):
    half_width = inputs.shape[-1] // 2
    return jnp.concatenate([-inputs[..., half_width:], inputs[..., :half_width]], axis=-1)

def unrotate(inputs):
    half_width = inputs.shape[-1] // 2
    return jnp.concatenate([inputs[..., half_width:], -inputs[..., :half_width]], axis=-1)

def to_rows(arr):
    model_width = arr.shape[3]
    return jnp.concatenate([arr[0].reshape(-1, model_width), arr[1][::-1].reshape(-1, model_width)], axis=0)

def to_layout(rows_arr, block_rows):
    half_len = rows_arr.shape[0] // 2
    model_width = rows_arr.shape[1]
    first_half = rows_arr[:half_len].reshape(-1, block_rows, model_width)
    second_half = rows_arr[half_len:].reshape(-1, block_rows, model_width)[::-1]
    return jnp.stack([first_half, second_half])

def barrier_bf(values):
    return lax.optimization_barrier(values.astype(jnp.bfloat16)).astype(jnp.float32)

def reference(block_input, dy, attn_gain, q_gain, k_gain, ffn_gain, wq, wk, wv, wo, w_gate, w_up, w_down):
    inputs = to_rows(block_input).astype(jnp.float32)
    cotangent = to_rows(dy)
    sequence_length = inputs.shape[0]
    query_group_size = QUERY_HEADS // KEY_VALUE_HEADS
    score_scale = 1.0 / math.sqrt(HEAD_SIZE)
    row_block = math.gcd(sequence_length, 256)
    positions = jnp.arange(sequence_length, dtype=jnp.int32)
    normed, inverse_in = rms_forward(inputs, attn_gain)
    normed_input_half = normed.astype(jnp.bfloat16)
    queries = jnp.dot(normed_input_half, wq, preferred_element_type=jnp.float32).reshape(sequence_length, QUERY_HEADS, HEAD_SIZE)
    key_unnormed = jnp.dot(normed_input_half, wk, preferred_element_type=jnp.float32).reshape(sequence_length, KEY_VALUE_HEADS, HEAD_SIZE)
    value_rows_half = jnp.dot(normed_input_half, wv, preferred_element_type=jnp.float32).astype(jnp.bfloat16)
    q_normed, q_inverse = rms_forward(queries, q_gain)
    k_normed, k_inverse = rms_forward(key_unnormed, k_gain)
    cosine, sine_tab = rope_tables(positions, HEAD_SIZE)
    query_rotated = (q_normed * cosine + rotate(q_normed) * sine_tab).astype(jnp.bfloat16)
    k_rot = (k_normed * cosine + rotate(k_normed) * sine_tab).astype(jnp.bfloat16)
    query_grouped = query_rotated.astype(jnp.float32).reshape(sequence_length, KEY_VALUE_HEADS, query_group_size, HEAD_SIZE)
    keys_f = k_rot.astype(jnp.float32)
    value_rows_wide = value_rows_half.astype(jnp.float32).reshape(sequence_length, KEY_VALUE_HEADS, HEAD_SIZE)

    def scores_of(row_start):
        query_block = lax.dynamic_slice_in_dim(query_grouped, row_start, row_block, 0)
        query_pos = row_start + jnp.arange(row_block, dtype=jnp.int32)
        scores = jnp.einsum('bngd,knd->ngbk', query_block, keys_f) * score_scale
        allowed = positions[None, :] <= query_pos[:, None]
        return (jnp.where(allowed, scores, -jnp.inf), query_block)

    def attend(running, row_start):
        scores, query_block = scores_of(row_start)
        row_max = lax.optimization_barrier(jnp.max(scores, axis=-1, keepdims=True))
        exp_scores = jnp.exp(scores - row_max)
        row_total = lax.optimization_barrier(jnp.sum(exp_scores, axis=-1, keepdims=True))
        probs_bf = barrier_bf(exp_scores)
        attn_blk = jnp.einsum('ngbk,knd->ngbd', probs_bf, value_rows_wide) / row_total
        log_total = (row_max + jnp.log(row_total))[..., 0]
        return (running, (jnp.transpose(attn_blk, (2, 0, 1, 3)), log_total))
    starts = jnp.arange(sequence_length // row_block, dtype=jnp.int32) * row_block
    _, (attention_block_list, log_totals) = lax.scan(attend, jnp.zeros((), jnp.float32), starts)
    attention_head_rows = attention_block_list.reshape(sequence_length, KEY_VALUE_HEADS, query_group_size, HEAD_SIZE)
    attn_bf = attention_head_rows.reshape(sequence_length, QUERY_HEADS * HEAD_SIZE).astype(jnp.bfloat16)
    residual = inputs + jnp.dot(attn_bf, wo, preferred_element_type=jnp.float32)
    ffn_normed, inverse_ffn = rms_forward(residual, ffn_gain)
    ffn_in = ffn_normed.astype(jnp.bfloat16)
    gate_pre = jnp.dot(ffn_in, w_gate, preferred_element_type=jnp.float32)
    up_pre = jnp.dot(ffn_in, w_up, preferred_element_type=jnp.float32)
    sigmoid_gate = jax.nn.sigmoid(gate_pre)
    silu_gate = gate_pre * sigmoid_gate
    hidden = (silu_gate * up_pre).astype(jnp.bfloat16)
    result = residual + jnp.dot(hidden, w_down, preferred_element_type=jnp.float32)
    d_w_down = jnp.dot(hidden.T, cotangent, preferred_element_type=jnp.float32)
    d_hidden = jnp.dot(cotangent, w_down.T, preferred_element_type=jnp.float32)
    d_gate = (d_hidden * up_pre * sigmoid_gate * (1.0 + gate_pre * (1.0 - sigmoid_gate))).astype(jnp.bfloat16)
    d_up = (d_hidden * silu_gate).astype(jnp.bfloat16)
    d_w_gate = jnp.dot(ffn_in.T, d_gate, preferred_element_type=jnp.float32)
    d_w_up = jnp.dot(ffn_in.T, d_up, preferred_element_type=jnp.float32)
    d_ffn_in = jnp.dot(d_gate, w_gate.T, preferred_element_type=jnp.float32) + jnp.dot(d_up, w_up.T, preferred_element_type=jnp.float32)
    d_res_norm, d_ffn_gain = rms_backward(residual, inverse_ffn, ffn_gain, d_ffn_in)
    d_residual = cotangent.astype(jnp.float32) + d_res_norm
    d_res_bf = d_residual.astype(jnp.bfloat16)
    d_wo = jnp.dot(attn_bf.T, d_res_bf, preferred_element_type=jnp.float32)
    attention_gradient = jnp.dot(d_res_bf, wo.T, preferred_element_type=jnp.float32).astype(jnp.bfloat16)
    output_gradient_wide = attention_gradient.astype(jnp.float32).reshape(sequence_length, KEY_VALUE_HEADS, query_group_size, HEAD_SIZE)
    delta_all = lax.optimization_barrier(jnp.sum(output_gradient_wide * attention_head_rows, axis=-1))

    def attend_back(running, block_inputs):
        grad_keys_acc, grad_values_acc = running
        row_start, log_total = block_inputs
        scores, query_block = scores_of(row_start)
        probs_f = jnp.exp(scores - log_total[..., None])
        grad_blk = lax.dynamic_slice_in_dim(output_gradient_wide, row_start, row_block, 0)
        delta_blk = jnp.transpose(lax.dynamic_slice_in_dim(delta_all, row_start, row_block, 0), (1, 2, 0))
        grad_probs = jnp.einsum('bngd,knd->ngbk', grad_blk, value_rows_wide)
        grad_scores = barrier_bf(probs_f * (grad_probs - delta_blk[..., None]) * score_scale)
        probs_bf = barrier_bf(probs_f)
        grad_query_blk = jnp.einsum('ngbk,knd->bngd', grad_scores, keys_f)
        grad_keys_acc = grad_keys_acc + jnp.einsum('ngbk,bngd->knd', grad_scores, query_block)
        grad_values_acc = grad_values_acc + jnp.einsum('ngbk,bngd->knd', probs_bf, grad_blk)
        return ((grad_keys_acc, grad_values_acc), grad_query_blk)
    empty_key_value = jnp.zeros((sequence_length, KEY_VALUE_HEADS, HEAD_SIZE), jnp.float32)
    (grad_keys_all, value_gradient_total), grad_query_blocks = lax.scan(attend_back, (empty_key_value, empty_key_value), (starts, log_totals))
    grad_q_rot = grad_query_blocks.reshape(sequence_length, QUERY_HEADS, HEAD_SIZE)
    d_q_normed = grad_q_rot * cosine + unrotate(grad_q_rot * sine_tab)
    d_queries, d_q_gain = rms_backward(queries, q_inverse, q_gain, d_q_normed)
    d_k_normed = grad_keys_all * cosine + unrotate(grad_keys_all * sine_tab)
    key_gradient, d_k_gain = rms_backward(key_unnormed, k_inverse, k_gain, d_k_normed)
    dq_bf = d_queries.reshape(sequence_length, QUERY_HEADS * HEAD_SIZE).astype(jnp.bfloat16)
    key_gradient_half = key_gradient.reshape(sequence_length, KEY_VALUE_HEADS * HEAD_SIZE).astype(jnp.bfloat16)
    value_gradient_half = value_gradient_total.reshape(sequence_length, KEY_VALUE_HEADS * HEAD_SIZE).astype(jnp.bfloat16)
    d_wq = jnp.dot(normed_input_half.T, dq_bf, preferred_element_type=jnp.float32)
    d_wk = jnp.dot(normed_input_half.T, key_gradient_half, preferred_element_type=jnp.float32)
    d_wv = jnp.dot(normed_input_half.T, value_gradient_half, preferred_element_type=jnp.float32)
    d_normed = jnp.dot(dq_bf, wq.T, preferred_element_type=jnp.float32)
    d_normed = d_normed + jnp.dot(key_gradient_half, wk.T, preferred_element_type=jnp.float32)
    d_normed = d_normed + jnp.dot(value_gradient_half, wv.T, preferred_element_type=jnp.float32)
    d_inputs, d_attn_gain = rms_backward(inputs, inverse_in, attn_gain, d_normed)
    grad_in = d_residual + d_inputs
    block_rows = block_input.shape[2]
    return (to_layout(result, block_rows).astype(jnp.bfloat16), to_layout(grad_in, block_rows), d_attn_gain, d_q_gain, d_k_gain, d_ffn_gain, d_wq, d_wk, d_wv, d_wo, d_w_gate, d_w_up, d_w_down)
```

```python
import functools
import math

import jax
import jax.numpy as jnp
from jax import lax
from jax.experimental import pallas as pl
from jax.experimental.pallas import tpu as pltpu
from jax.sharding import Mesh
from jax.sharding import PartitionSpec as P

EPS = 1e-05
ROPE_BASE = 1000000.0
F32 = jnp.float32
BF16 = jnp.bfloat16
HEAD = 64
BLOCK = 128
GROUP = ("inner", "fsdp")
EVERY = ("outer", "inner", "fsdp")


def dot(a, b, dims=((1,), (0,))):
    return lax.dot_general(a, b, (dims, ((), ())), preferred_element_type=F32)


def rms_forward(inputs, gain_vec):
    inverse = lax.rsqrt(jnp.mean(inputs * inputs, axis=-1, keepdims=True) + EPS)
    return (inputs * inverse * gain_vec, inverse)


def rms_backward(inputs, inverse, gain_vec, grad_out):
    scaled = grad_out * gain_vec
    inner_mean = jnp.mean(scaled * inputs, axis=-1, keepdims=True)
    grad_in = inverse * scaled - inputs * (inverse * inverse * inverse) * inner_mean
    grad_gain = jnp.sum((grad_out * inputs * inverse).reshape(-1, inputs.shape[-1]), axis=0)
    return (grad_in, grad_gain)


def rope_tables(positions, head_width):
    frequency = ROPE_BASE ** (-2.0 * jnp.arange(head_width // 2, dtype=F32) / head_width)
    angles = positions.astype(F32)[:, None] * frequency[None, :]
    cosine = jnp.concatenate([jnp.cos(angles), jnp.cos(angles)], axis=-1)[:, None, :]
    sine_tab = jnp.concatenate([jnp.sin(angles), jnp.sin(angles)], axis=-1)[:, None, :]
    return (cosine, sine_tab)


def rotate(inputs):
    half_width = inputs.shape[-1] // 2
    return jnp.concatenate([-inputs[..., half_width:], inputs[..., :half_width]], axis=-1)


def unrotate(inputs):
    half_width = inputs.shape[-1] // 2
    return jnp.concatenate([inputs[..., half_width:], -inputs[..., :half_width]], axis=-1)


SCORE = 1.0 / math.sqrt(HEAD)
SCORE2 = SCORE * math.log2(math.e)


def attn_fwd_kernel(steps, outer_ref, qt_ref, kv_ref, out_ref, total_ref):
    outer = outer_ref[0]
    half = kv_ref.shape[0] // (2 * steps)
    sub = half // 2
    wide = 2 * sub

    def block(rows, size, cols, mask, acc, total):
        kv = kv_ref[pl.ds(pl.multiple_of(rows, sub), size), :]
        probs = jnp.exp2(dot(kv, qt_ref[:, cols]) * SCORE2)
        if mask is not None:
            probs = jnp.where(mask, probs, 0.0)
        total = total + jnp.sum(probs.reshape(size // 8, 8, wide), axis=0)
        acc = acc + dot(kv, probs.astype(BF16), ((0,), (0,)))
        return acc, total

    key = lax.broadcasted_iota(jnp.int32, (sub, wide), 0)
    query = lax.broadcasted_iota(jnp.int32, (sub, wide), 1) % sub
    diagonal = key <= query
    for late in range(2):
        for part in range(2):
            cols = pl.ds((late * 2 + part) * wide, wide)

            def full(m, carry):
                if late:
                    rows = jnp.where(m < steps, m * 2, (outer + 1 + m - steps) * 2 + 1) * half
                else:
                    rows = m * 2 * half
                return block(rows, half, cols, None, *carry)

            count = 2 * steps - 1 - outer if late else outer
            own = (outer * 2 + late) * half
            carry = (jnp.zeros((2 * HEAD, wide), F32), jnp.zeros((8, wide), F32))
            carry = lax.fori_loop(0, count, full, carry)
            if part:
                carry = block(own, sub, cols, None, *carry)
            acc, total = block(own + part * sub, sub, cols, diagonal, *carry)
            total = jnp.sum(total, axis=0, keepdims=True)
            out_ref[:, cols] = acc[HEAD:] / total
            total_ref[:, cols] = jnp.log2(total)


def attn_bwd_kernel(
    steps, outer_ref, qt_ref, q_ref, gt_ref, g_ref, kv_ref, log_ref, delta_ref, dq_ref, dkv_ref
):
    outer = outer_ref[0]
    half = kv_ref.shape[0] // (2 * steps)
    sub = half // 2
    wide = 2 * sub
    dkv_ref[...] = jnp.zeros_like(dkv_ref)

    def block(rows, size, cols, mask, acc):
        rows = pl.ds(pl.multiple_of(rows, sub), size)
        kv = kv_ref[rows, :]
        probs = jnp.exp2(dot(kv, qt_ref[:, cols]) * SCORE2 - log_ref[:, cols])
        if mask is not None:
            probs = jnp.where(mask, probs, 0.0)
        grads = dot(kv, gt_ref[:, cols])
        grads = (probs * (grads - delta_ref[:, cols]) * SCORE).astype(BF16)
        dkv_ref[rows, :] += dot(grads, q_ref[cols, :]) + dot(probs.astype(BF16), g_ref[cols, :])
        return acc + dot(kv, grads, ((0,), (0,)))

    key = lax.broadcasted_iota(jnp.int32, (sub, wide), 0)
    query = lax.broadcasted_iota(jnp.int32, (sub, wide), 1) % sub
    diagonal = key <= query
    for late in range(2):
        for part in range(2):
            cols = pl.ds((late * 2 + part) * wide, wide)

            def full(m, acc):
                if late:
                    rows = jnp.where(m < steps, m * 2, (outer + 1 + m - steps) * 2 + 1) * half
                else:
                    rows = m * 2 * half
                return block(rows, half, cols, None, acc)

            count = 2 * steps - 1 - outer if late else outer
            own = (outer * 2 + late) * half
            acc = lax.fori_loop(0, count, full, jnp.zeros((2 * HEAD, wide), F32))
            if part:
                acc = block(own, sub, cols, None, acc)
            acc = block(own + part * sub, sub, cols, diagonal, acc)
            dq_ref[:, cols] = acc[:HEAD]


SMEM = pl.BlockSpec(memory_space=pltpu.SMEM)
VMEM = pl.BlockSpec(memory_space=pltpu.VMEM)


def attn_fwd(outer, qt, kv, steps):
    cols = qt.shape[1]
    work = kv.shape[0] * cols // 2
    return pl.pallas_call(
        functools.partial(attn_fwd_kernel, steps),
        out_shape=(
            jax.ShapeDtypeStruct((HEAD, cols), F32),
            jax.ShapeDtypeStruct((1, cols), F32),
        ),
        in_specs=[SMEM, VMEM, VMEM],
        out_specs=[VMEM, VMEM],
        cost_estimate=pl.CostEstimate(
            flops=work * 512, transcendentals=work, bytes_accessed=4 << 20
        ),
        name="attn_fwd",
    )(outer, qt, kv)


def attn_bwd(outer, qt, q, gt, g, kv, log_total, delta, steps):
    cols = qt.shape[1]
    work = kv.shape[0] * cols // 2
    return pl.pallas_call(
        functools.partial(attn_bwd_kernel, steps),
        out_shape=(
            jax.ShapeDtypeStruct((HEAD, cols), F32),
            jax.ShapeDtypeStruct(kv.shape, F32),
        ),
        in_specs=[SMEM] + [VMEM] * 7,
        out_specs=[VMEM, VMEM],
        cost_estimate=pl.CostEstimate(
            flops=work * 1280, transcendentals=work, bytes_accessed=8 << 20
        ),
        name="attn_bwd",
    )(outer, qt, q, gt, g, kv, log_total, delta)


def swap(array, axis_size):
    return lax.ppermute(array, "fsdp", [(k, (k + 1) % axis_size) for k in range(axis_size)])


def local(
    block_input, dy, attn_gain, q_gain, k_gain, ffn_gain, wq, wk, wv, wo, w_gate, w_up, w_down
):
    steps = lax.axis_size("outer")
    inner_size = lax.axis_size("inner")
    fsdp_size = lax.axis_size("fsdp")
    outer = lax.axis_index("outer")
    inner = lax.axis_index("inner")
    fsdp = lax.axis_index("fsdp")
    group = inner_size * fsdp_size
    lane = fsdp * inner_size + inner
    part = block_input.shape[2]
    width = block_input.shape[3]
    block_len = part * fsdp_size
    rows = 2 * part
    half = inner_size * block_len
    pairs = steps * inner_size
    kv_heads = group

    def gather(arr):
        arr = lax.all_gather(arr.reshape(2, part, -1), GROUP, axis=0, tiled=False)
        arr = arr.reshape(inner_size, fsdp_size, 2, part, -1)
        early = arr[:, :, 0].reshape(half, -1)
        late = arr[::-1, :, 1].reshape(half, -1)
        return jnp.concatenate([early, late], axis=0)

    def by_device(arr):
        early = arr[:half].reshape(inner_size, fsdp_size, part, -1)
        late = arr[half:].reshape(inner_size, fsdp_size, part, -1)[::-1]
        return jnp.stack([early, late], axis=2).reshape(group, rows, -1)

    def scatter(arr):
        return lax.psum_scatter(by_device(arr), GROUP, scatter_dimension=0, tiled=False)

    def heads_to_tokens(arr):
        got = lax.all_to_all(by_device(arr), GROUP, split_axis=0, concat_axis=0, tiled=True)
        got = got.reshape(inner_size, fsdp_size, rows, -1)
        return jnp.transpose(got, (2, 1, 0, 3)).reshape(rows, -1)

    def tokens_to_heads(arr):
        cut = arr.reshape(rows, fsdp_size, inner_size, -1)
        cut = jnp.transpose(cut, (2, 1, 0, 3)).reshape(group, rows, -1)
        got = lax.all_to_all(cut, GROUP, split_axis=0, concat_axis=0, tiled=True)
        got = got.reshape(inner_size, fsdp_size, 2, part, -1)
        early = got[:, :, 0].reshape(half, -1)
        late = got[::-1, :, 1].reshape(half, -1)
        return jnp.concatenate([early, late], axis=0)

    def join(mine, other):
        return jnp.where(
            fsdp == 0,
            jnp.concatenate([mine, other], axis=0),
            jnp.concatenate([other, mine], axis=0),
        )

    def cols_of(arr, start, size):
        return lax.dynamic_slice_in_dim(arr, start, size, 1)

    def slice_exchange(arr, start, other_start, size):
        mine = cols_of(arr, start, size)
        return join(mine, swap(cols_of(arr, other_start, size), fsdp_size))

    other_lane = (1 - fsdp) * inner_size + inner

    qkv = lambda n: jnp.concatenate(
        [
            cols_of(wq, n * 2 * HEAD, 2 * HEAD),
            cols_of(wk, n * HEAD, HEAD),
            cols_of(wv, n * HEAD, HEAD),
        ],
        axis=1,
    )
    w_qkv = join(qkv(lane), swap(qkv(other_lane), fsdp_size))
    wo_all = join(wo, swap(wo, fsdp_size))
    ff = w_gate.shape[1]
    tiles = 2 * ff // group // BLOCK
    reach = (tiles + 1) // 2 * BLOCK
    own_ff = ff // group
    step_ff = (tiles // 2) * BLOCK

    def ff_start(f):
        return ((f * inner_size + inner) // 2) * tiles * BLOCK + (inner % 2) * step_ff

    gate_w = slice_exchange(w_gate, ff_start(fsdp), ff_start(1 - fsdp), reach)
    up_w = slice_exchange(w_up, ff_start(fsdp), ff_start(1 - fsdp), reach)
    down_start = (inner // 2) * tiles * BLOCK + (inner % 2) * step_ff
    down_w = lax.dynamic_slice_in_dim(w_down, down_start, reach, 0)
    col = jnp.arange(reach, dtype=jnp.int32)
    pad = reach - own_ff
    valid = jnp.where(inner % 2 == 0, col < own_ff, col >= pad)[None, :]

    wq_all = join(wq, swap(wq, fsdp_size))
    wk_all = join(wk, swap(wk, fsdp_size))
    wv_all = join(wv, swap(wv, fsdp_size))

    inputs = block_input.reshape(rows, width).astype(F32)
    cotangent = dy.reshape(rows, width)
    cot_group = gather(cotangent)
    normed, inverse_in = rms_forward(inputs, attn_gain)
    normed_group = gather(normed.astype(BF16))
    proj = dot(normed_group, w_qkv)
    queries = proj[:, : 2 * HEAD].reshape(2 * half, 2, HEAD)
    key_unnormed = proj[:, 2 * HEAD : 3 * HEAD].reshape(2 * half, 1, HEAD)
    value_rows = proj[:, 3 * HEAD :].astype(BF16)
    q_normed, q_inverse = rms_forward(queries, q_gain)
    k_normed, k_inverse = rms_forward(key_unnormed, k_gain)
    within = jnp.arange(half, dtype=jnp.int32)
    positions = jnp.concatenate(
        [outer * half + within, (2 * steps - 1 - outer) * half + within], axis=0
    )
    cosine, sine_tab = rope_tables(positions, HEAD)
    q_rot = (q_normed * cosine + rotate(q_normed) * sine_tab).astype(BF16)
    k_rot = (k_normed * cosine + rotate(k_normed) * sine_tab).astype(BF16)
    kv_own = jnp.concatenate([k_rot[:, 0], value_rows], axis=1)
    kv = lax.all_gather(kv_own, "outer", axis=0, tiled=True)

    sub = half // 2

    def to_cols(arr):
        return jnp.transpose(arr.reshape(2, 2, sub, 2, -1), (0, 1, 3, 2, 4)).reshape(4 * half, -1)

    def from_cols(arr):
        return jnp.transpose(arr.reshape(2, 2, 2, sub, -1), (0, 1, 3, 2, 4)).reshape(2 * half, -1)

    q_cols = jnp.pad(to_cols(q_rot), ((0, 0), (0, HEAD)))
    q_t = q_cols.T
    outer_arr = outer.reshape(1)
    attn_t, log2_total = attn_fwd(outer_arr, q_t, kv, steps)
    attn = from_cols(attn_t.T)
    attn_bf = attn.astype(BF16)
    attn_rows = heads_to_tokens(attn_bf)
    residual = inputs + dot(attn_rows, wo_all)
    ffn_normed, inverse_ffn = rms_forward(residual, ffn_gain)
    ffn_in = gather(ffn_normed.astype(BF16))
    gate_pre = dot(ffn_in, gate_w)
    up_pre = dot(ffn_in, up_w)
    sigmoid_gate = jax.nn.sigmoid(gate_pre)
    silu_gate = gate_pre * sigmoid_gate
    hidden = jnp.where(valid, silu_gate * up_pre, 0.0).astype(BF16)
    result = residual + scatter(dot(hidden, down_w))

    d_hidden = jnp.where(valid, dot(cot_group, down_w, ((1,), (1,))), 0.0)
    d_gate = (d_hidden * up_pre * sigmoid_gate * (1.0 + gate_pre * (1.0 - sigmoid_gate))).astype(
        BF16
    )
    d_up = (d_hidden * silu_gate).astype(BF16)
    d_ffn_in = scatter(dot(d_gate, gate_w, ((1,), (1,))) + dot(d_up, up_w, ((1,), (1,))))
    d_w_down = dot(hidden, cot_group, ((0,), (0,)))
    d_w_gate = dot(ffn_in, d_gate, ((0,), (0,)))
    d_w_up = dot(ffn_in, d_up, ((0,), (0,)))
    d_res_norm, d_ffn_gain = rms_backward(residual, inverse_ffn, ffn_gain, d_ffn_in)
    d_residual = cotangent.astype(F32) + d_res_norm
    d_res_bf = d_residual.astype(BF16)
    attn_grad = tokens_to_heads(dot(d_res_bf, wo_all, ((1,), (1,))).astype(BF16))
    d_res_group = gather(d_res_bf)
    d_wo = dot(attn_bf, d_res_group, ((0,), (0,)))
    delta = jnp.sum((attn_grad.astype(F32) * attn).reshape(2 * half, 2, HEAD), axis=-1)
    g_cols = jnp.pad(to_cols(attn_grad.reshape(2 * half, 2, HEAD)), ((0, 0), (HEAD, 0)))
    delta_cols = to_cols(delta[..., None]).reshape(1, 4 * half)
    dq_t, d_kv = attn_bwd(
        outer_arr, q_t, q_cols, g_cols.T, g_cols, kv, log2_total, delta_cols, steps
    )
    d_kv = lax.psum_scatter(d_kv, "outer", scatter_dimension=0, tiled=True)
    grad_q_rot = from_cols(dq_t.T).reshape(2 * half, 2, HEAD)
    grad_k_rot = d_kv[:, :HEAD].reshape(2 * half, 1, HEAD)
    d_q_normed = grad_q_rot * cosine + unrotate(grad_q_rot * sine_tab)
    d_queries, d_q_gain = rms_backward(queries, q_inverse, q_gain, d_q_normed)
    d_k_normed = grad_k_rot * cosine + unrotate(grad_k_rot * sine_tab)
    d_keys, d_k_gain = rms_backward(key_unnormed, k_inverse, k_gain, d_k_normed)
    d_qkv = jnp.concatenate(
        [d_queries.reshape(2 * half, 2 * HEAD), d_keys[:, 0], d_kv[:, HEAD:]], axis=1
    ).astype(BF16)
    d_w_qkv = dot(normed_group, d_qkv, ((0,), (0,)))
    rows_qkv = heads_to_tokens(d_qkv).reshape(rows, group, 4 * HEAD)
    dq_rows = rows_qkv[:, :, : 2 * HEAD].reshape(rows, -1)
    dk_rows = rows_qkv[:, :, 2 * HEAD : 3 * HEAD].reshape(rows, -1)
    dv_rows = rows_qkv[:, :, 3 * HEAD :].reshape(rows, -1)
    d_normed = dot(dq_rows, wq_all, ((1,), (1,)))
    d_normed = d_normed + dot(dk_rows, wk_all, ((1,), (1,)))
    d_normed = d_normed + dot(dv_rows, wv_all, ((1,), (1,)))
    d_inputs, d_attn_gain = rms_backward(inputs, inverse_in, attn_gain, d_normed)
    grad_in = d_residual + d_inputs

    def rows_out(arr):
        part_sum = lax.psum_scatter(arr, "outer", scatter_dimension=0, tiled=True)
        got = lax.all_to_all(part_sum, GROUP, split_axis=0, concat_axis=0, tiled=True)
        got = got.reshape(inner_size, fsdp_size, -1, arr.shape[1])
        return jnp.transpose(got, (1, 0, 2, 3)).reshape(group, -1, arr.shape[1])

    def windows(arr):
        pair = arr.reshape(group // 2, 2, arr.shape[1], reach)
        first, second = pair[:, 0], pair[:, 1]
        whole = jnp.concatenate(
            [
                first[..., :step_ff],
                first[..., step_ff:] + second[..., : reach - step_ff],
                second[..., reach - step_ff :],
            ],
            axis=-1,
        )
        return jnp.transpose(whole, (1, 0, 2)).reshape(arr.shape[1], ff)

    own_gate = windows(rows_out(d_w_gate))
    own_up = windows(rows_out(d_w_up))
    own_qkv = jnp.transpose(rows_out(d_w_qkv), (1, 0, 2))
    own_q = own_qkv[:, :, : 2 * HEAD].reshape(-1, wq.shape[1])
    own_k = own_qkv[:, :, 2 * HEAD : 3 * HEAD].reshape(-1, wk.shape[1])
    own_v = own_qkv[:, :, 3 * HEAD :].reshape(-1, wv.shape[1])
    down_rows = lax.dynamic_slice_in_dim(d_w_down, jnp.where(inner % 2 == 0, 0, pad), own_ff, 0)
    down_sum = lax.psum_scatter(down_rows, "outer", scatter_dimension=0, tiled=True)
    wo_sum = lax.psum_scatter(d_wo, "outer", scatter_dimension=0, tiled=True)
    moves = []
    for z in range(steps):
        for i in range(inner_size):
            for f in range(fsdp_size):
                moves.append((z * group + i * fsdp_size + f, steps * (f * inner_size + i) + z))
    moved = lax.ppermute(jnp.concatenate([down_sum, wo_sum], axis=0), EVERY, moves)
    own_down = moved[: down_sum.shape[0]]
    own_o = moved[down_sum.shape[0] :]
    gains = lax.psum(
        jnp.concatenate([d_attn_gain, d_ffn_gain, jnp.pad(d_q_gain, (0, 0)), d_k_gain]), EVERY
    )
    return (
        result.astype(BF16).reshape(block_input.shape),
        grad_in.reshape(block_input.shape),
        gains[:width],
        gains[2 * width : 2 * width + HEAD],
        gains[2 * width + HEAD :],
        gains[width : 2 * width],
        own_q,
        own_k,
        own_v,
        own_o,
        own_gate,
        own_up,
        own_down,
    )


def solution(mesh):
    ctx, fsdp = mesh.shape["ctx"], mesh.shape["fsdp"]
    inner = 8 // fsdp
    grid = Mesh(mesh.devices.reshape(ctx // inner, inner, fsdp), EVERY)
    tokens = P(None, ("outer", "inner"), "fsdp", None)
    shard = P("fsdp", None)
    owned = P(EVERY, None)
    return jax.shard_map(
        local,
        mesh=grid,
        in_specs=(tokens, tokens) + (P(),) * 4 + (shard,) * 7,
        out_specs=(tokens, tokens) + (P(),) * 4 + (owned,) * 7,
        check_vma=False,
    )
```

```python
import functools
import math

import jax
import jax.numpy as jnp
from jax import lax
from jax.experimental import pallas as pl
from jax.experimental.pallas import tpu as pltpu
from jax.sharding import Mesh
from jax.sharding import PartitionSpec as P

EPS = 1e-05
ROPE_BASE = 1000000.0
F32 = jnp.float32
BF16 = jnp.bfloat16
HEAD = 64
BLOCK = 128
GROUP = ("inner", "fsdp")
EVERY = ("outer", "inner", "fsdp")


def dot(a, b, dims=((1,), (0,))):
    return lax.dot_general(a, b, (dims, ((), ())), preferred_element_type=F32)


def rms_forward(inputs, gain_vec):
    inverse = lax.rsqrt(jnp.mean(inputs * inputs, axis=-1, keepdims=True) + EPS)
    return (inputs * inverse * gain_vec, inverse)


def rms_backward(inputs, inverse, gain_vec, grad_out):
    scaled = grad_out * gain_vec
    inner_mean = jnp.mean(scaled * inputs, axis=-1, keepdims=True)
    grad_in = inverse * scaled - inputs * (inverse * inverse * inverse) * inner_mean
    grad_gain = jnp.sum((grad_out * inputs * inverse).reshape(-1, inputs.shape[-1]), axis=0)
    return (grad_in, grad_gain)


def rope_tables(positions, head_width):
    frequency = ROPE_BASE ** (-2.0 * jnp.arange(head_width // 2, dtype=F32) / head_width)
    angles = positions.astype(F32)[:, None] * frequency[None, :]
    cosine = jnp.concatenate([jnp.cos(angles), jnp.cos(angles)], axis=-1)[:, None, :]
    sine_tab = jnp.concatenate([jnp.sin(angles), jnp.sin(angles)], axis=-1)[:, None, :]
    return (cosine, sine_tab)


def rotate(inputs):
    half_width = inputs.shape[-1] // 2
    return jnp.concatenate([-inputs[..., half_width:], inputs[..., :half_width]], axis=-1)


def unrotate(inputs):
    half_width = inputs.shape[-1] // 2
    return jnp.concatenate([inputs[..., half_width:], -inputs[..., :half_width]], axis=-1)


SCORE = 1.0 / math.sqrt(HEAD)
SCORE2 = SCORE * math.log2(math.e)


def attn_bwd_kernel(
    steps, outer_ref, qt_ref, q_ref, gt_ref, g_ref, kv_ref, log_ref, delta_ref, dq_ref, dkv_ref
):
    outer = outer_ref[0]
    half = kv_ref.shape[0] // (2 * steps)
    sub = half // 2
    wide = 2 * sub
    dkv_ref[...] = jnp.zeros_like(dkv_ref)

    def block(rows, size, cols, mask, acc):
        rows = pl.ds(pl.multiple_of(rows, sub), size)
        kv = kv_ref[rows, :]
        probs = jnp.exp2(dot(kv, qt_ref[:, cols]) * SCORE2 - log_ref[:, cols])
        if mask is not None:
            probs = jnp.where(mask, probs, 0.0)
        grads = dot(kv, gt_ref[:, cols])
        grads = (probs * (grads - delta_ref[:, cols]) * SCORE).astype(BF16)
        dkv_ref[rows, :] += dot(grads, q_ref[cols, :]) + dot(probs.astype(BF16), g_ref[cols, :])
        return acc + dot(kv, grads, ((0,), (0,)))

    key = lax.broadcasted_iota(jnp.int32, (sub, wide), 0)
    query = lax.broadcasted_iota(jnp.int32, (sub, wide), 1) % sub
    diagonal = key <= query
    for late in range(2):
        for part in range(2):
            cols = pl.ds((late * 2 + part) * wide, wide)

            def full(m, acc):
                if late:
                    rows = jnp.where(m < steps, m * 2, (outer + 1 + m - steps) * 2 + 1) * half
                else:
                    rows = m * 2 * half
                return block(rows, half, cols, None, acc)

            count = 2 * steps - 1 - outer if late else outer
            own = (outer * 2 + late) * half
            acc = lax.fori_loop(0, count, full, jnp.zeros((2 * HEAD, wide), F32))
            if part:
                acc = block(own, sub, cols, None, acc)
            acc = block(own + part * sub, sub, cols, diagonal, acc)
            dq_ref[:, cols] = acc[:HEAD]


def place():
    outer, inner, fsdp = (lax.axis_index(name) for name in EVERY)
    return outer, inner, fsdp


def remote(src, dst, send, recv, device):
    return pltpu.make_async_remote_copy(
        src_ref=src,
        dst_ref=dst,
        send_sem=send,
        recv_sem=recv,
        device_id=device,
        device_id_type=pl.DeviceIdType.MESH,
    )


def greet(devices):
    barrier = pltpu.get_barrier_semaphore()
    for device in devices:
        pl.semaphore_signal(
            barrier, inc=1, device_id=device, device_id_type=pl.DeviceIdType.MESH
        )
    return lambda: pl.semaphore_wait(barrier, len(devices))


def chip_peer(k):
    outer, inner, fsdp = place()
    chip = ((inner // 2) * 2 + fsdp + k) % 4
    return (outer, (chip // 2) * 2 + inner % 2, chip % 2)


def sibling():
    outer, inner, fsdp = place()
    return (outer, inner + 1 - 2 * (inner % 2), fsdp)


def group_peer(k):
    outer, inner, fsdp = place()
    member = (inner * 2 + fsdp + k) % 8
    return (outer, member // 2, member % 2)


def member_of(device):
    return device[1] * 2 + device[2]


def early_row(member, part):
    return pl.multiple_of(member * part, part)


def late_row(member, part):
    return pl.multiple_of((3 - member // 2) * 2 * part + (member % 2) * part, part)


class Gather:
    def __init__(self, own, land, send, recv):
        self.own, self.land, self.send, self.recv = own, land, send, recv
        self.mine = member_of(place())
        self.started = []

    def copy(self, src, member, piece, slot, device):
        dst = self.land(member)[piece]
        copy = remote(
            src, dst, self.send.at[piece, slot], self.recv.at[piece, member], device
        )
        copy.start()
        self.started.append(copy)

    def start(self):
        for k in (1, 2, 3, 0):
            device = chip_peer(k) if k else sibling()
            for piece, src in enumerate(self.own):
                self.copy(src, self.mine, piece, k, device)

    def wait(self, member):
        for piece, dst in enumerate(self.land(member)):
            remote(
                dst, dst, self.send.at[piece, 0], self.recv.at[piece, member], sibling()
            ).wait_recv()

    def pass_on(self, k):
        member = member_of(chip_peer(k))
        self.wait(member)
        for piece, dst in enumerate(self.land(member)):
            self.copy(dst, member, piece, 3 + k, sibling())
        return member

    def others(self):
        near = sibling()
        yield member_of(near)
        for k in (1, 2, 3):
            chip = ((near[1] // 2) * 2 + near[2] + k) % 4
            yield ((chip // 2) * 2 + near[1] % 2) * 2 + chip % 2

    def drain(self):
        for copy in self.started:
            copy.wait_send()


def rms_rows(values, gain):
    inverse = lax.rsqrt(jnp.mean(values * values, axis=-1, keepdims=True) + EPS)
    return values * inverse * gain


def head_inverse(values, low):
    squares = values * values
    first = jnp.sum(jnp.where(low, squares, 0.0), axis=-1, keepdims=True)
    second = jnp.sum(jnp.where(low, 0.0, squares), axis=-1, keepdims=True)
    return jnp.where(
        low, lax.rsqrt(first * (1.0 / HEAD) + EPS), lax.rsqrt(second * (1.0 / HEAD) + EPS)
    )


def halves(values, front):
    quarter = HEAD // 2
    return jnp.where(
        front,
        pltpu.roll(values, values.shape[-1] - quarter, 1),
        pltpu.roll(values, quarter, 1),
    )


def front_kernel(
    x_ref,
    gain_ref,
    mine_ref,
    other_ref,
    cos_ref,
    sin_ref,
    qg_ref,
    kg_ref,
    normed_out,
    proj_ref,
    q_ref,
    qt_ref,
    kv_ref,
    own,
    land,
    send,
    recv,
    out_sem,
):
    _, _, fsdp = place()
    part = x_ref.shape[1]
    half = land.shape[1]
    width = land.shape[2]
    sub = half // 2
    depth = width // 2
    ready = greet([sibling()] + [chip_peer(k) for k in (1, 2, 3)])
    for late in range(2):
        rows = x_ref[late].astype(F32)
        own[late] = rms_rows(rows, gain_ref[...]).astype(BF16)
    ready()

    def slots(member):
        return [
            land.at[0, pl.ds(early_row(member, part), part)],
            land.at[1, pl.ds(late_row(member, part), part)],
        ]

    gather = Gather([own.at[0], own.at[1]], slots, send, recv)
    gather.start()
    member = member_of(place())
    land[0, pl.ds(early_row(member, part), part)] = own[0]
    land[1, pl.ds(late_row(member, part), part)] = own[1]
    for k in (1, 3, 2):
        gather.pass_on(k)
    for member in gather.others():
        gather.wait(member)
    out = pltpu.make_async_copy(land, normed_out, out_sem)
    out.start()

    lane = lax.broadcasted_iota(jnp.int32, (sub, 2 * HEAD), 1)
    low = lane < HEAD
    front = lane % HEAD < HEAD // 2
    mine_at = pl.ds(pl.multiple_of(fsdp * depth, depth), depth)
    other_at = pl.ds(pl.multiple_of((1 - fsdp) * depth, depth), depth)

    @pl.loop(0, 4)
    def _(tile):
        late = tile // 2
        inside = pl.ds(pl.multiple_of((tile % 2) * sub, sub), sub)
        rows = pl.ds(pl.multiple_of(tile * sub, sub), sub)
        proj = dot(land[late, inside, mine_at], mine_ref[...])
        proj = proj + dot(land[late, inside, other_at], other_ref[...])
        proj_ref[rows, :] = proj
        cos, sin = cos_ref[rows, :], sin_ref[rows, :]
        raw = proj[:, : 2 * HEAD]
        normed = raw * head_inverse(raw, low) * qg_ref[...]
        rotated = normed * cos + halves(normed, front) * sin
        second = pltpu.roll(rotated, HEAD, 1)
        for head, values in enumerate((rotated, second)):
            values = jnp.where(low, values, 0.0)
            cols = pl.ds(pl.multiple_of(tile * 2 * sub + head * sub, sub), sub)
            q_ref[cols, :] = values.astype(BF16)
            qt_ref[:, cols] = values.T.astype(BF16)
        raw = proj[:, 2 * HEAD :]
        normed = raw * head_inverse(raw, low) * kg_ref[...]
        rotated = normed * cos + halves(normed, front) * sin
        kv_ref[rows, :] = jnp.where(low, rotated, raw).astype(BF16)

    gather.drain()
    out.wait()


def middle_kernel(
    steps,
    x_ref,
    dy_ref,
    qt_ref,
    kv_ref,
    wo_mine,
    wo_other,
    gain_ref,
    kv_out,
    cot_out,
    attn_t_ref,
    log_ref,
    attn_ref,
    residual_ref,
    ffn_ref,
    kv_all,
    acc_ref,
    total_ref,
    token_rows,
    dy_send,
    dy_recv,
    kv_send,
    kv_recv,
    swap_send,
    swap_recv,
    out_sem,
):
    outer, inner, fsdp = place()
    me = member_of((outer, inner, fsdp))
    part = x_ref.shape[1]
    half = kv_ref.shape[0] // 2
    sub = half // 2
    wide = 2 * sub
    width = x_ref.shape[2]
    depth = width // 2

    def outer_peer(k):
        return ((outer + k) % steps, inner, fsdp)

    ready = greet(
        [outer_peer(k) for k in range(1, steps)] + [group_peer(k) for k in range(1, 8)]
    )
    kv_all[outer] = kv_ref[...]
    acc_ref[...] = jnp.zeros_like(acc_ref)
    total_ref[...] = jnp.zeros_like(total_ref)
    ready()
    for k in range(1, steps):
        remote(
            kv_ref, kv_all.at[outer], kv_send.at[k], kv_recv.at[outer], outer_peer(steps - k)
        ).start()
    cot = Gather(
        [dy_ref.at[n] for n in range(2)],
        lambda member: [cot_out.at[member, n] for n in range(2)],
        dy_send,
        dy_recv,
    )
    cot.start()
    own_dy = pltpu.make_async_copy(dy_ref, cot_out.at[me], out_sem.at[0])
    own_dy.start()

    def block(slot, row, size, col, mask):
        kv = kv_all[slot, pl.ds(pl.multiple_of(row, sub), size), :]
        cols = pl.ds(pl.multiple_of(col, wide), wide)
        probs = jnp.exp2(dot(kv, qt_ref[:, cols]) * SCORE2)
        if mask is not None:
            probs = jnp.where(mask, probs, 0.0)
        total_ref[:, cols] += jnp.sum(probs.reshape(size // 8, 8, wide), axis=0)
        acc_ref[:, cols] += dot(kv, probs.astype(BF16), ((0,), (0,)))

    key = lax.broadcasted_iota(jnp.int32, (sub, wide), 0)
    query = lax.broadcasted_iota(jnp.int32, (sub, wide), 1) % sub
    diagonal = key <= query

    @pl.loop(0, 2)
    def _(late):
        block(outer, late * half, sub, late * 2 * wide, diagonal)
        block(outer, late * half, sub, late * 2 * wide + wide, None)
        block(outer, late * half + sub, sub, late * 2 * wide + wide, diagonal)

    @pl.loop(0, 2)
    def _(n):
        block(outer, 0, half, (2 + n) * wide, None)

    @pl.loop(1, steps)
    def _(k):
        slot = (outer + k) % steps
        late = jnp.where(slot < outer, 0, 1)
        remote(
            kv_ref, kv_all.at[slot], kv_send.at[k], kv_recv.at[slot], outer_peer(k)
        ).wait_recv()

        @pl.loop(0, 2)
        def _(n):
            block(slot, 0, half, (2 + n) * wide, None)
            block(slot, late * half, half, (late * 2 + n) * wide, None)

    kv_copy = pltpu.make_async_copy(kv_all, kv_out, out_sem.at[1])
    kv_copy.start()

    @pl.loop(0, 4)
    def _(tile):
        heads = []
        for head in range(2):
            cols = pl.ds(pl.multiple_of(tile * wide + head * sub, sub), sub)
            total = jnp.sum(total_ref[:, cols], axis=0, keepdims=True)
            values = acc_ref[HEAD:, cols] / total
            attn_t_ref[:, cols] = values
            log_ref[:, cols] = jnp.log2(total)
            heads.append(values)
        inside = pl.ds(pl.multiple_of((tile % 2) * sub, sub), sub)
        attn_ref[tile // 2, inside, :] = jnp.concatenate(heads, axis=0).T.astype(BF16)

    lane = fsdp * 4 + inner

    def chunk(member):
        return [
            attn_ref.at[0, pl.ds(early_row(member, part), part)],
            attn_ref.at[1, pl.ds(late_row(member, part), part)],
        ]

    def landing(source):
        cols = pl.ds(pl.multiple_of(source * 2 * HEAD, 2 * HEAD), 2 * HEAD)
        return [token_rows.at[n, :, cols] for n in range(2)]

    swaps = []
    for k in range(1, 8):
        device = group_peer(k)
        for n in range(2):
            swaps.append(
                remote(
                    chunk(member_of(device))[n],
                    landing(lane)[n],
                    swap_send.at[n, k],
                    swap_recv.at[n, lane],
                    device,
                )
            )
            swaps[-1].start()
    own_cols = pl.ds(pl.multiple_of(lane * 2 * HEAD, 2 * HEAD), 2 * HEAD)
    token_rows[0, :, own_cols] = attn_ref[0, pl.ds(early_row(me, part), part), :]
    token_rows[1, :, own_cols] = attn_ref[1, pl.ds(late_row(me, part), part), :]
    for k in range(1, 8):
        device = group_peer(k)
        source = device[2] * 4 + device[1]
        for n in range(2):
            remote(
                landing(source)[n],
                landing(source)[n],
                swap_send.at[n, k],
                swap_recv.at[n, source],
                device,
            ).wait_recv()

    mine_at = pl.ds(pl.multiple_of(fsdp * depth, depth), depth)
    other_at = pl.ds(pl.multiple_of((1 - fsdp) * depth, depth), depth)
    for n in range(2):
        values = dot(token_rows[n, :, mine_at], wo_mine[...])
        values = values + dot(token_rows[n, :, other_at], wo_other[...])
        values = values + x_ref[n].astype(F32)
        residual_ref[n] = values
        ffn_ref[n] = rms_rows(values, gain_ref[...]).astype(BF16)

    for k in (1, 3, 2):
        cot.pass_on(k)
    for member in cot.others():
        cot.wait(member)
    cot.drain()
    for copy in swaps:
        copy.wait_send()
    for k in range(1, steps):
        remote(
            kv_ref, kv_all.at[outer], kv_send.at[k], kv_recv.at[outer], outer_peer(steps - k)
        ).wait_send()
    own_dy.wait()
    kv_copy.wait()


SMEM = pl.BlockSpec(memory_space=pltpu.SMEM)
VMEM = pl.BlockSpec(memory_space=pltpu.VMEM)
ANY = pl.BlockSpec(memory_space=pl.ANY)
DMA = pltpu.SemaphoreType.DMA


def params(collective):
    return pltpu.CompilerParams(
        collective_id=collective, has_side_effects=True, vmem_limit_bytes=60 << 20
    )


def front(x, gain, mine, other, cos, sin, q_gain, k_gain):
    part, width = x.shape[1:]
    tokens = cos.shape[0]
    half = tokens // 2
    return pl.pallas_call(
        front_kernel,
        out_shape=(
            jax.ShapeDtypeStruct((2, half, width), BF16),
            jax.ShapeDtypeStruct((tokens, 4 * HEAD), F32),
            jax.ShapeDtypeStruct((2 * tokens, 2 * HEAD), BF16),
            jax.ShapeDtypeStruct((2 * HEAD, 2 * tokens), BF16),
            jax.ShapeDtypeStruct((tokens, 2 * HEAD), BF16),
        ),
        in_specs=[VMEM] * 8,
        out_specs=[ANY, VMEM, VMEM, VMEM, VMEM],
        scratch_shapes=[
            pltpu.VMEM((2, part, width), BF16),
            pltpu.VMEM((2, half, width), BF16),
            DMA((2, 8)),
            DMA((2, 8)),
            DMA,
        ],
        compiler_params=params(0),
        name="front",
    )(x, gain, mine, other, cos, sin, q_gain, k_gain)


def middle(x, dy, qt, kv, wo_mine, wo_other, gain, steps):
    part, width = x.shape[1:]
    tokens = kv.shape[0]
    half = tokens // 2
    return pl.pallas_call(
        functools.partial(middle_kernel, steps),
        out_shape=(
            jax.ShapeDtypeStruct((steps, tokens, 2 * HEAD), BF16),
            jax.ShapeDtypeStruct((8, 2, part, width), BF16),
            jax.ShapeDtypeStruct((HEAD, 2 * tokens), F32),
            jax.ShapeDtypeStruct((1, 2 * tokens), F32),
            jax.ShapeDtypeStruct((2, half, 2 * HEAD), BF16),
            jax.ShapeDtypeStruct((2, part, width), F32),
            jax.ShapeDtypeStruct((2, part, width), BF16),
        ),
        in_specs=[VMEM] * 7,
        out_specs=[ANY, ANY] + [VMEM] * 5,
        scratch_shapes=[
            pltpu.VMEM((steps, tokens, 2 * HEAD), BF16),
            pltpu.VMEM((2 * HEAD, 2 * tokens), F32),
            pltpu.VMEM((8, 2 * tokens), F32),
            pltpu.VMEM((2, part, width), BF16),
            DMA((2, 8)),
            DMA((2, 8)),
            DMA((steps,)),
            DMA((steps,)),
            DMA((2, 8)),
            DMA((2, 8)),
            DMA((2,)),
        ],
        compiler_params=params(1),
        name="middle",
    )(x, dy, qt, kv, wo_mine, wo_other, gain)


def attn_bwd(outer, qt, q, gt, g, kv, log_total, delta, steps):
    cols = qt.shape[1]
    work = kv.shape[0] * cols // 2
    return pl.pallas_call(
        functools.partial(attn_bwd_kernel, steps),
        out_shape=(
            jax.ShapeDtypeStruct((HEAD, cols), F32),
            jax.ShapeDtypeStruct(kv.shape, F32),
        ),
        in_specs=[SMEM] + [VMEM] * 7,
        out_specs=[VMEM, VMEM],
        cost_estimate=pl.CostEstimate(
            flops=work * 1280, transcendentals=work, bytes_accessed=8 << 20
        ),
        name="attn_bwd",
    )(outer, qt, q, gt, g, kv, log_total, delta)


def swap(array, axis_size):
    return lax.ppermute(array, "fsdp", [(k, (k + 1) % axis_size) for k in range(axis_size)])


def local(
    block_input, dy, attn_gain, q_gain, k_gain, ffn_gain, wq, wk, wv, wo, w_gate, w_up, w_down
):
    steps = lax.axis_size("outer")
    inner_size = lax.axis_size("inner")
    fsdp_size = lax.axis_size("fsdp")
    outer = lax.axis_index("outer")
    inner = lax.axis_index("inner")
    fsdp = lax.axis_index("fsdp")
    group = inner_size * fsdp_size
    lane = fsdp * inner_size + inner
    part = block_input.shape[2]
    width = block_input.shape[3]
    block_len = part * fsdp_size
    rows = 2 * part
    half = inner_size * block_len
    pairs = steps * inner_size
    kv_heads = group

    def gather(arr):
        arr = lax.all_gather(arr.reshape(2, part, -1), GROUP, axis=0, tiled=False)
        arr = arr.reshape(inner_size, fsdp_size, 2, part, -1)
        early = arr[:, :, 0].reshape(half, -1)
        late = arr[::-1, :, 1].reshape(half, -1)
        return jnp.concatenate([early, late], axis=0)

    def by_device(arr):
        early = arr[:half].reshape(inner_size, fsdp_size, part, -1)
        late = arr[half:].reshape(inner_size, fsdp_size, part, -1)[::-1]
        return jnp.stack([early, late], axis=2).reshape(group, rows, -1)

    def scatter(arr):
        return lax.psum_scatter(by_device(arr), GROUP, scatter_dimension=0, tiled=False)

    def heads_to_tokens(arr):
        got = lax.all_to_all(by_device(arr), GROUP, split_axis=0, concat_axis=0, tiled=True)
        got = got.reshape(inner_size, fsdp_size, rows, -1)
        return jnp.transpose(got, (2, 1, 0, 3)).reshape(rows, -1)

    def tokens_to_heads(arr):
        cut = arr.reshape(rows, fsdp_size, inner_size, -1)
        cut = jnp.transpose(cut, (2, 1, 0, 3)).reshape(group, rows, -1)
        got = lax.all_to_all(cut, GROUP, split_axis=0, concat_axis=0, tiled=True)
        got = got.reshape(inner_size, fsdp_size, 2, part, -1)
        early = got[:, :, 0].reshape(half, -1)
        late = got[::-1, :, 1].reshape(half, -1)
        return jnp.concatenate([early, late], axis=0)

    def join(mine, other):
        return jnp.where(
            fsdp == 0,
            jnp.concatenate([mine, other], axis=0),
            jnp.concatenate([other, mine], axis=0),
        )

    def cols_of(arr, start, size):
        return lax.dynamic_slice_in_dim(arr, start, size, 1)

    def slice_exchange(arr, start, other_start, size):
        mine = cols_of(arr, start, size)
        return join(mine, swap(cols_of(arr, other_start, size), fsdp_size))

    other_lane = (1 - fsdp) * inner_size + inner

    qkv = lambda n: jnp.concatenate(
        [
            cols_of(wq, n * 2 * HEAD, 2 * HEAD),
            cols_of(wk, n * HEAD, HEAD),
            cols_of(wv, n * HEAD, HEAD),
        ],
        axis=1,
    )
    qkv_mine = qkv(lane)
    qkv_other = swap(qkv(other_lane), fsdp_size)
    wo_other = swap(wo, fsdp_size)
    wo_all = join(wo, wo_other)
    ff = w_gate.shape[1]
    tiles = 2 * ff // group // BLOCK
    reach = (tiles + 1) // 2 * BLOCK
    own_ff = ff // group
    step_ff = (tiles // 2) * BLOCK

    def ff_start(f):
        return ((f * inner_size + inner) // 2) * tiles * BLOCK + (inner % 2) * step_ff

    gate_w = slice_exchange(w_gate, ff_start(fsdp), ff_start(1 - fsdp), reach)
    up_w = slice_exchange(w_up, ff_start(fsdp), ff_start(1 - fsdp), reach)
    down_start = (inner // 2) * tiles * BLOCK + (inner % 2) * step_ff
    down_w = lax.dynamic_slice_in_dim(w_down, down_start, reach, 0)
    col = jnp.arange(reach, dtype=jnp.int32)
    pad = reach - own_ff
    valid = jnp.where(inner % 2 == 0, col < own_ff, col >= pad)[None, :]

    wq_all = join(wq, swap(wq, fsdp_size))
    wk_all = join(wk, swap(wk, fsdp_size))
    wv_all = join(wv, swap(wv, fsdp_size))

    x = block_input.reshape(2, part, width)
    inputs = x.reshape(rows, width).astype(F32)
    cotangent = dy.reshape(rows, width)
    within = jnp.arange(half, dtype=jnp.int32)
    positions = jnp.concatenate(
        [outer * half + within, (2 * steps - 1 - outer) * half + within], axis=0
    )
    cosine, sine_tab = rope_tables(positions, HEAD)
    front_sign = jnp.where(jnp.arange(HEAD) < HEAD // 2, -1.0, 1.0).astype(F32)
    cos2 = jnp.tile(cosine[:, 0], (1, 2))
    sin2 = jnp.tile(sine_tab[:, 0] * front_sign, (1, 2))
    q_gain2 = jnp.tile(q_gain, 2)[None]
    k_gain2 = jnp.tile(k_gain, 2)[None]
    normed_group, proj, q_cols, q_t, kv_own = front(
        x, attn_gain[None], qkv_mine, qkv_other, cos2, sin2, q_gain2, k_gain2
    )
    normed_group = normed_group.reshape(2 * half, width)
    kv, cot_group, attn_t, log2_total, attn_bf, residual, ffn_rows = middle(
        x, dy.reshape(2, part, width), q_t, kv_own, wo, wo_other, ffn_gain[None], steps
    )
    kv = kv.reshape(-1, 2 * HEAD)
    cot_group = cot_group.reshape(group * rows, width)
    attn_bf = attn_bf.reshape(2 * half, 2 * HEAD)
    residual = residual.reshape(rows, width)
    inverse_ffn = lax.rsqrt(jnp.mean(residual * residual, axis=-1, keepdims=True) + EPS)
    inverse_in = lax.rsqrt(jnp.mean(inputs * inputs, axis=-1, keepdims=True) + EPS)
    queries = proj[:, : 2 * HEAD].reshape(2 * half, 2, HEAD)
    key_unnormed = proj[:, 2 * HEAD : 3 * HEAD].reshape(2 * half, 1, HEAD)
    q_inverse = lax.rsqrt(jnp.mean(queries * queries, axis=-1, keepdims=True) + EPS)
    k_inverse = lax.rsqrt(
        jnp.mean(key_unnormed * key_unnormed, axis=-1, keepdims=True) + EPS
    )
    sub = half // 2

    def to_cols(arr):
        return jnp.transpose(arr.reshape(2, 2, sub, 2, -1), (0, 1, 3, 2, 4)).reshape(4 * half, -1)

    def from_cols(arr):
        return jnp.transpose(arr.reshape(2, 2, 2, sub, -1), (0, 1, 3, 2, 4)).reshape(2 * half, -1)

    outer_arr = outer.reshape(1)
    attn = from_cols(attn_t.T)
    ffn_in = lax.all_gather(ffn_rows.reshape(rows, width), GROUP, axis=0, tiled=True)

    def scatter_members(arr):
        return lax.psum_scatter(
            arr.reshape(group, rows, width), GROUP, scatter_dimension=0, tiled=False
        )

    gate_pre = dot(ffn_in, gate_w)
    up_pre = dot(ffn_in, up_w)
    sigmoid_gate = jax.nn.sigmoid(gate_pre)
    silu_gate = gate_pre * sigmoid_gate
    hidden = jnp.where(valid, silu_gate * up_pre, 0.0).astype(BF16)
    result = residual + scatter_members(dot(hidden, down_w))

    d_hidden = jnp.where(valid, dot(cot_group, down_w, ((1,), (1,))), 0.0)
    d_gate = (d_hidden * up_pre * sigmoid_gate * (1.0 + gate_pre * (1.0 - sigmoid_gate))).astype(
        BF16
    )
    d_up = (d_hidden * silu_gate).astype(BF16)
    d_ffn_in = scatter_members(dot(d_gate, gate_w, ((1,), (1,))) + dot(d_up, up_w, ((1,), (1,))))
    d_w_down = dot(hidden, cot_group, ((0,), (0,)))
    d_w_gate = dot(ffn_in, d_gate, ((0,), (0,)))
    d_w_up = dot(ffn_in, d_up, ((0,), (0,)))
    d_res_norm, d_ffn_gain = rms_backward(residual, inverse_ffn, ffn_gain, d_ffn_in)
    d_residual = cotangent.astype(F32) + d_res_norm
    d_res_bf = d_residual.astype(BF16)
    attn_grad = tokens_to_heads(dot(d_res_bf, wo_all, ((1,), (1,))).astype(BF16))
    d_res_group = gather(d_res_bf)
    d_wo = dot(attn_bf, d_res_group, ((0,), (0,)))
    delta = jnp.sum((attn_grad.astype(F32) * attn).reshape(2 * half, 2, HEAD), axis=-1)
    g_cols = jnp.pad(to_cols(attn_grad.reshape(2 * half, 2, HEAD)), ((0, 0), (HEAD, 0)))
    delta_cols = to_cols(delta[..., None]).reshape(1, 4 * half)
    dq_t, d_kv = attn_bwd(
        outer_arr, q_t, q_cols, g_cols.T, g_cols, kv, log2_total, delta_cols, steps
    )
    d_kv = lax.psum_scatter(d_kv, "outer", scatter_dimension=0, tiled=True)
    grad_q_rot = from_cols(dq_t.T).reshape(2 * half, 2, HEAD)
    grad_k_rot = d_kv[:, :HEAD].reshape(2 * half, 1, HEAD)
    d_q_normed = grad_q_rot * cosine + unrotate(grad_q_rot * sine_tab)
    d_queries, d_q_gain = rms_backward(queries, q_inverse, q_gain, d_q_normed)
    d_k_normed = grad_k_rot * cosine + unrotate(grad_k_rot * sine_tab)
    d_keys, d_k_gain = rms_backward(key_unnormed, k_inverse, k_gain, d_k_normed)
    d_qkv = jnp.concatenate(
        [d_queries.reshape(2 * half, 2 * HEAD), d_keys[:, 0], d_kv[:, HEAD:]], axis=1
    ).astype(BF16)
    d_w_qkv = dot(normed_group, d_qkv, ((0,), (0,)))
    rows_qkv = heads_to_tokens(d_qkv).reshape(rows, group, 4 * HEAD)
    dq_rows = rows_qkv[:, :, : 2 * HEAD].reshape(rows, -1)
    dk_rows = rows_qkv[:, :, 2 * HEAD : 3 * HEAD].reshape(rows, -1)
    dv_rows = rows_qkv[:, :, 3 * HEAD :].reshape(rows, -1)
    d_normed = dot(dq_rows, wq_all, ((1,), (1,)))
    d_normed = d_normed + dot(dk_rows, wk_all, ((1,), (1,)))
    d_normed = d_normed + dot(dv_rows, wv_all, ((1,), (1,)))
    d_inputs, d_attn_gain = rms_backward(inputs, inverse_in, attn_gain, d_normed)
    grad_in = d_residual + d_inputs

    def rows_out(arr):
        part_sum = lax.psum_scatter(arr, "outer", scatter_dimension=0, tiled=True)
        got = lax.all_to_all(part_sum, GROUP, split_axis=0, concat_axis=0, tiled=True)
        got = got.reshape(inner_size, fsdp_size, -1, arr.shape[1])
        return jnp.transpose(got, (1, 0, 2, 3)).reshape(group, -1, arr.shape[1])

    def windows(arr):
        pair = arr.reshape(group // 2, 2, arr.shape[1], reach)
        first, second = pair[:, 0], pair[:, 1]
        whole = jnp.concatenate(
            [
                first[..., :step_ff],
                first[..., step_ff:] + second[..., : reach - step_ff],
                second[..., reach - step_ff :],
            ],
            axis=-1,
        )
        return jnp.transpose(whole, (1, 0, 2)).reshape(arr.shape[1], ff)

    own_gate = windows(rows_out(d_w_gate))
    own_up = windows(rows_out(d_w_up))
    own_qkv = jnp.transpose(rows_out(d_w_qkv), (1, 0, 2))
    own_q = own_qkv[:, :, : 2 * HEAD].reshape(-1, wq.shape[1])
    own_k = own_qkv[:, :, 2 * HEAD : 3 * HEAD].reshape(-1, wk.shape[1])
    own_v = own_qkv[:, :, 3 * HEAD :].reshape(-1, wv.shape[1])
    down_rows = lax.dynamic_slice_in_dim(d_w_down, jnp.where(inner % 2 == 0, 0, pad), own_ff, 0)
    down_sum = lax.psum_scatter(down_rows, "outer", scatter_dimension=0, tiled=True)
    wo_sum = lax.psum_scatter(d_wo, "outer", scatter_dimension=0, tiled=True)
    moves = []
    for z in range(steps):
        for i in range(inner_size):
            for f in range(fsdp_size):
                moves.append((z * group + i * fsdp_size + f, steps * (f * inner_size + i) + z))
    moved = lax.ppermute(jnp.concatenate([down_sum, wo_sum], axis=0), EVERY, moves)
    own_down = moved[: down_sum.shape[0]]
    own_o = moved[down_sum.shape[0] :]
    gains = lax.psum(
        jnp.concatenate([d_attn_gain, d_ffn_gain, jnp.pad(d_q_gain, (0, 0)), d_k_gain]), EVERY
    )
    return (
        result.astype(BF16).reshape(block_input.shape),
        grad_in.reshape(block_input.shape),
        gains[:width],
        gains[2 * width : 2 * width + HEAD],
        gains[2 * width + HEAD :],
        gains[width : 2 * width],
        own_q,
        own_k,
        own_v,
        own_o,
        own_gate,
        own_up,
        own_down,
    )


def solution(mesh):
    ctx, fsdp = mesh.shape["ctx"], mesh.shape["fsdp"]
    inner = 8 // fsdp
    grid = Mesh(mesh.devices.reshape(ctx // inner, inner, fsdp), EVERY)
    tokens = P(None, ("outer", "inner"), "fsdp", None)
    shard = P("fsdp", None)
    owned = P(EVERY, None)
    return jax.shard_map(
        local,
        mesh=grid,
        in_specs=(tokens, tokens) + (P(),) * 4 + (shard,) * 7,
        out_specs=(tokens, tokens) + (P(),) * 4 + (owned,) * 7,
        check_vma=False,
    )
```

```python
import functools
import math

import jax
import jax.numpy as jnp
from jax import lax
from jax.experimental import pallas as pl
from jax.experimental.pallas import tpu as pltpu
from jax.sharding import Mesh
from jax.sharding import PartitionSpec as P

EPS = 1e-05
ROPE_BASE = 1000000.0
F32 = jnp.float32
BF16 = jnp.bfloat16
HEAD = 64
BLOCK = 128
GROUP = ("inner", "fsdp")
EVERY = ("outer", "inner", "fsdp")


def dot(a, b, dims=((1,), (0,))):
    return lax.dot_general(a, b, (dims, ((), ())), preferred_element_type=F32)


SCORE = 1.0 / math.sqrt(HEAD)
SCORE2 = SCORE * math.log2(math.e)


def place():
    outer, inner, fsdp = (lax.axis_index(name) for name in EVERY)
    return outer, inner, fsdp


def remote(src, dst, send, recv, device):
    return pltpu.make_async_remote_copy(
        src_ref=src,
        dst_ref=dst,
        send_sem=send,
        recv_sem=recv,
        device_id=device,
        device_id_type=pl.DeviceIdType.MESH,
    )


def greet(devices):
    barrier = pltpu.get_barrier_semaphore()
    for device in devices:
        pl.semaphore_signal(
            barrier, inc=1, device_id=device, device_id_type=pl.DeviceIdType.MESH
        )
    return lambda: pl.semaphore_wait(barrier, len(devices))


def chip_peer(k, other_core=0):
    outer, inner, fsdp = place()
    chip = ((inner // 2) * 2 + fsdp + k) % 4
    return (outer, (chip // 2) * 2 + (inner + other_core) % 2, chip % 2)


def sibling():
    outer, inner, fsdp = place()
    return (outer, inner + 1 - 2 * (inner % 2), fsdp)


def group_peer(k):
    outer, inner, fsdp = place()
    member = (inner * 2 + fsdp + k) % 8
    return (outer, member // 2, member % 2)


def member_of(device):
    return device[1] * 2 + device[2]


def slot_of(device):
    return ((device[1] // 2) * 2 + device[2]) * 2 + device[1] % 2


def early_row(member, part):
    return pl.multiple_of(member * part, part)


def late_row(member, part):
    return pl.multiple_of((3 - member // 2) * 2 * part + (member % 2) * part, part)


class Gather:
    def __init__(self, own, land, send, recv):
        self.own, self.land, self.send, self.recv = own, land, send, recv
        self.pieces = range(len(own))

    def copy(self, src, owner, piece, slot, device):
        return remote(
            src,
            self.land(owner)[piece],
            self.send.at[piece, slot],
            self.recv.at[piece, slot_of(owner)],
            device,
        )

    def start(self):
        for k in (1, 2, 3, 0):
            device = chip_peer(k) if k else sibling()
            for piece in self.pieces:
                self.copy(self.own[piece], place(), piece, k, device).start()

    def wait(self, owner):
        for piece in self.pieces:
            dst = self.land(owner)[piece]
            self.copy(dst, owner, piece, 0, sibling()).wait_recv()

    def pass_on(self, k):
        owner = chip_peer(k)
        self.wait(owner)
        for piece in self.pieces:
            self.copy(self.land(owner)[piece], owner, piece, 4 + k, sibling()).start()

    def far(self, k):
        return chip_peer(k, 1)

    def finish(self):
        self.wait(self.far(0))
        for k in (1, 2, 3):
            self.wait(self.far(k))

    def drain(self):
        for slot in (0, 1, 2, 3, 5, 6, 7):
            for piece in self.pieces:
                self.copy(self.own[piece], place(), piece, slot, sibling()).wait_send()


def rms_rows(values, gain):
    inverse = lax.rsqrt(jnp.mean(values * values, axis=-1, keepdims=True) + EPS)
    return values * inverse * gain


def head_inverse(values, low):
    squares = values * values
    first = jnp.sum(jnp.where(low, squares, 0.0), axis=-1, keepdims=True)
    second = jnp.sum(jnp.where(low, 0.0, squares), axis=-1, keepdims=True)
    return jnp.where(
        low, lax.rsqrt(first * (1.0 / HEAD) + EPS), lax.rsqrt(second * (1.0 / HEAD) + EPS)
    )


def halves(values, front):
    quarter = HEAD // 2
    return jnp.where(
        front,
        pltpu.roll(values, values.shape[-1] - quarter, 1),
        pltpu.roll(values, quarter, 1),
    )


def front_kernel(
    x_ref,
    gain_ref,
    weights_any,
    far_any,
    cos_ref,
    sin_ref,
    qg_ref,
    kg_ref,
    normed_out,
    proj_ref,
    q_ref,
    qt_ref,
    kv_ref,
    own,
    land,
    mine_ref,
    other_ref,
    send,
    recv,
    load_sem,
    out_sem,
):
    _, inner, fsdp = place()
    cols = 4 * HEAD
    at = pl.ds(pl.multiple_of((fsdp * 4 + inner) * cols, cols), cols)
    loads = [
        pltpu.make_async_copy(weights_any.at[:, at], mine_ref, load_sem.at[0]),
        pltpu.make_async_copy(far_any, other_ref, load_sem.at[1]),
    ]
    for copy in loads:
        copy.start()
    part = x_ref.shape[1]
    half = land.shape[1]
    width = land.shape[2]
    sub = half // 2
    depth = width // 2
    ready = greet([sibling()] + [chip_peer(k) for k in (1, 2, 3)])
    for late in range(2):
        rows = x_ref[late].astype(F32)
        own[late] = rms_rows(rows, gain_ref[...]).astype(BF16)
    ready()

    def slots(device):
        member = member_of(device)
        return [
            land.at[0, pl.ds(early_row(member, part), part)],
            land.at[1, pl.ds(late_row(member, part), part)],
        ]

    gather = Gather([own.at[0], own.at[1]], slots, send, recv)
    gather.start()
    member = member_of(place())
    land[0, pl.ds(early_row(member, part), part)] = own[0]
    land[1, pl.ds(late_row(member, part), part)] = own[1]
    for k in (1, 3, 2):
        gather.pass_on(k)
    gather.finish()
    out = pltpu.make_async_copy(land, normed_out, out_sem)
    out.start()
    for copy in loads:
        copy.wait()

    lane = lax.broadcasted_iota(jnp.int32, (sub, 2 * HEAD), 1)
    low = lane < HEAD
    front = lane % HEAD < HEAD // 2
    mine_at = pl.ds(pl.multiple_of(fsdp * depth, depth), depth)
    other_at = pl.ds(pl.multiple_of((1 - fsdp) * depth, depth), depth)

    @pl.loop(0, 4)
    def _(tile):
        late = tile // 2
        inside = pl.ds(pl.multiple_of((tile % 2) * sub, sub), sub)
        rows = pl.ds(pl.multiple_of(tile * sub, sub), sub)
        proj = dot(land[late, inside, mine_at], mine_ref[...])
        proj = proj + dot(land[late, inside, other_at], other_ref[...])
        proj_ref[rows, :] = proj
        cos, sin = cos_ref[rows, :], sin_ref[rows, :]
        raw = proj[:, : 2 * HEAD]
        normed = raw * head_inverse(raw, low) * qg_ref[...]
        rotated = normed * cos + halves(normed, front) * sin
        second = pltpu.roll(rotated, HEAD, 1)
        for head, values in enumerate((rotated, second)):
            values = jnp.where(low, values, 0.0)
            cols = pl.ds(pl.multiple_of(tile * 2 * sub + head * sub, sub), sub)
            q_ref[cols, :] = values.astype(BF16)
            qt_ref[:, cols] = values.T.astype(BF16)
        raw = proj[:, 2 * HEAD :]
        normed = raw * head_inverse(raw, low) * kg_ref[...]
        rotated = normed * cos + halves(normed, front) * sin
        kv_ref[rows, :] = jnp.where(low, rotated, raw).astype(BF16)

    gather.drain()
    out.wait()


def middle_kernel(
    steps,
    x_ref,
    dy_ref,
    qt_ref,
    kv_ref,
    wo_mine,
    wo_other,
    gain_ref,
    kv_out,
    cot_out,
    attn_t_ref,
    log_ref,
    attn_ref,
    residual_ref,
    ffn_ref,
    kv_all,
    acc_ref,
    total_ref,
    token_rows,
    dy_send,
    dy_recv,
    kv_send,
    kv_recv,
    swap_send,
    swap_recv,
    out_sem,
):
    outer, inner, fsdp = place()
    me = member_of((outer, inner, fsdp))
    part = x_ref.shape[1]
    half = kv_ref.shape[0] // 2
    sub = half // 2
    wide = 2 * sub
    width = x_ref.shape[2]
    depth = width // 2

    def outer_peer(k):
        return ((outer + k) % steps, inner, fsdp)

    ready = greet(
        [outer_peer(k) for k in range(1, steps)] + [group_peer(k) for k in range(1, 8)]
    )
    kv_all[outer] = kv_ref[...]
    acc_ref[...] = jnp.zeros_like(acc_ref)
    total_ref[...] = jnp.zeros_like(total_ref)
    ready()
    for k in range(1, steps):
        remote(
            kv_ref, kv_all.at[outer], kv_send.at[k], kv_recv.at[outer], outer_peer(steps - k)
        ).start()
    cot = Gather(
        [dy_ref.at[n] for n in range(2)],
        lambda device: [cot_out.at[slot_of(device), n] for n in range(2)],
        dy_send,
        dy_recv,
    )
    cot.start()
    own_dy = pltpu.make_async_copy(dy_ref, cot_out.at[slot_of(place())], out_sem.at[0])
    own_dy.start()

    def block(slot, row, size, col, mask):
        kv = kv_all[slot, pl.ds(pl.multiple_of(row, sub), size), :]
        cols = pl.ds(pl.multiple_of(col, wide), wide)
        probs = jnp.exp2(dot(kv, qt_ref[:, cols]) * SCORE2)
        if mask is not None:
            probs = jnp.where(mask, probs, 0.0)
        total_ref[:, cols] += jnp.sum(probs.reshape(size // 8, 8, wide), axis=0)
        acc_ref[:, cols] += dot(kv, probs.astype(BF16), ((0,), (0,)))

    key = lax.broadcasted_iota(jnp.int32, (sub, wide), 0)
    query = lax.broadcasted_iota(jnp.int32, (sub, wide), 1) % sub
    diagonal = key <= query

    @pl.loop(0, 2)
    def _(late):
        block(outer, late * half, sub, late * 2 * wide, diagonal)
        block(outer, late * half, sub, late * 2 * wide + wide, None)
        block(outer, late * half + sub, sub, late * 2 * wide + wide, diagonal)

    @pl.loop(0, 2)
    def _(n):
        block(outer, 0, half, (2 + n) * wide, None)

    @pl.loop(1, steps)
    def _(k):
        slot = (outer + k) % steps
        late = jnp.where(slot < outer, 0, 1)
        remote(
            kv_ref, kv_all.at[slot], kv_send.at[k], kv_recv.at[slot], outer_peer(k)
        ).wait_recv()

        @pl.loop(0, 2)
        def _(n):
            block(slot, 0, half, (2 + n) * wide, None)
            block(slot, late * half, half, (late * 2 + n) * wide, None)

    kv_copy = pltpu.make_async_copy(kv_all, kv_out, out_sem.at[1])
    kv_copy.start()

    @pl.loop(0, 4)
    def _(tile):
        heads = []
        for head in range(2):
            cols = pl.ds(pl.multiple_of(tile * wide + head * sub, sub), sub)
            total = jnp.sum(total_ref[:, cols], axis=0, keepdims=True)
            values = acc_ref[HEAD:, cols] / total
            attn_t_ref[:, cols] = values
            log_ref[:, cols] = jnp.log2(total)
            heads.append(values)
        inside = pl.ds(pl.multiple_of((tile % 2) * sub, sub), sub)
        attn_ref[tile // 2, inside, :] = jnp.concatenate(heads, axis=0).T.astype(BF16)

    lane = fsdp * 4 + inner

    def chunk(member):
        return [
            attn_ref.at[0, pl.ds(early_row(member, part), part)],
            attn_ref.at[1, pl.ds(late_row(member, part), part)],
        ]

    def landing(source):
        cols = pl.ds(pl.multiple_of(source * 2 * HEAD, 2 * HEAD), 2 * HEAD)
        return [token_rows.at[n, :, cols] for n in range(2)]

    swaps = []
    for k in range(1, 8):
        device = group_peer(k)
        for n in range(2):
            swaps.append(
                remote(
                    chunk(member_of(device))[n],
                    landing(lane)[n],
                    swap_send.at[n, k],
                    swap_recv.at[n, lane],
                    device,
                )
            )
            swaps[-1].start()
    own_cols = pl.ds(pl.multiple_of(lane * 2 * HEAD, 2 * HEAD), 2 * HEAD)
    token_rows[0, :, own_cols] = attn_ref[0, pl.ds(early_row(me, part), part), :]
    token_rows[1, :, own_cols] = attn_ref[1, pl.ds(late_row(me, part), part), :]
    for k in range(1, 8):
        device = group_peer(k)
        source = device[2] * 4 + device[1]
        for n in range(2):
            remote(
                landing(source)[n],
                landing(source)[n],
                swap_send.at[n, k],
                swap_recv.at[n, source],
                device,
            ).wait_recv()

    mine_at = pl.ds(pl.multiple_of(fsdp * depth, depth), depth)
    other_at = pl.ds(pl.multiple_of((1 - fsdp) * depth, depth), depth)
    for n in range(2):
        values = dot(token_rows[n, :, mine_at], wo_mine[...])
        values = values + dot(token_rows[n, :, other_at], wo_other[...])
        values = values + x_ref[n].astype(F32)
        residual_ref[n] = values
        ffn_ref[n] = rms_rows(values, gain_ref[...]).astype(BF16)

    for k in (1, 3, 2):
        cot.pass_on(k)
    cot.finish()
    cot.drain()
    for copy in swaps:
        copy.wait_send()
    for k in range(1, steps):
        remote(
            kv_ref, kv_all.at[outer], kv_send.at[k], kv_recv.at[outer], outer_peer(steps - k)
        ).wait_send()
    own_dy.wait()
    kv_copy.wait()


SMEM = pl.BlockSpec(memory_space=pltpu.SMEM)
VMEM = pl.BlockSpec(memory_space=pltpu.VMEM)
ANY = pl.BlockSpec(memory_space=pl.ANY)
DMA = pltpu.SemaphoreType.DMA


def params(collective):
    return pltpu.CompilerParams(
        collective_id=collective, has_side_effects=True, vmem_limit_bytes=60 << 20
    )


def front(x, gain, weights, far, cos, sin, q_gain, k_gain):
    part, width = x.shape[1:]
    tokens = cos.shape[0]
    half = tokens // 2
    return pl.pallas_call(
        front_kernel,
        out_shape=(
            jax.ShapeDtypeStruct((2, half, width), BF16),
            jax.ShapeDtypeStruct((tokens, 4 * HEAD), F32),
            jax.ShapeDtypeStruct((2 * tokens, 2 * HEAD), BF16),
            jax.ShapeDtypeStruct((2 * HEAD, 2 * tokens), BF16),
            jax.ShapeDtypeStruct((tokens, 2 * HEAD), BF16),
        ),
        in_specs=[VMEM] * 2 + [ANY] * 2 + [VMEM] * 4,
        out_specs=[ANY, VMEM, VMEM, VMEM, VMEM],
        scratch_shapes=[
            pltpu.VMEM((2, part, width), BF16),
            pltpu.VMEM((2, half, width), BF16),
            pltpu.VMEM(far.shape, BF16),
            pltpu.VMEM(far.shape, BF16),
            DMA((2, 8)),
            DMA((2, 8)),
            DMA((2,)),
            DMA,
        ],
        compiler_params=params(0),
        name="front",
    )(x, gain, weights, far, cos, sin, q_gain, k_gain)


def middle(x, dy, qt, kv, wo_mine, wo_other, gain, steps):
    part, width = x.shape[1:]
    tokens = kv.shape[0]
    half = tokens // 2
    return pl.pallas_call(
        functools.partial(middle_kernel, steps),
        out_shape=(
            jax.ShapeDtypeStruct((steps, tokens, 2 * HEAD), BF16),
            jax.ShapeDtypeStruct((8, 2, part, width), BF16),
            jax.ShapeDtypeStruct((HEAD, 2 * tokens), F32),
            jax.ShapeDtypeStruct((1, 2 * tokens), F32),
            jax.ShapeDtypeStruct((2, half, 2 * HEAD), BF16),
            jax.ShapeDtypeStruct((2, part, width), F32),
            jax.ShapeDtypeStruct((2, part, width), BF16),
        ),
        in_specs=[VMEM] * 7,
        out_specs=[ANY, ANY] + [VMEM] * 5,
        scratch_shapes=[
            pltpu.VMEM((steps, tokens, 2 * HEAD), BF16),
            pltpu.VMEM((2 * HEAD, 2 * tokens), F32),
            pltpu.VMEM((8, 2 * tokens), F32),
            pltpu.VMEM((2, part, width), BF16),
            DMA((2, 8)),
            DMA((2, 8)),
            DMA((steps,)),
            DMA((steps,)),
            DMA((2, 8)),
            DMA((2, 8)),
            DMA((2,)),
        ],
        compiler_params=params(1),
        name="middle",
    )(x, dy, qt, kv, wo_mine, wo_other, gain)


def ffn_kernel(
    steps,
    ffn_ref,
    residual_ref,
    dy_ref,
    attn_ref,
    gain_ref,
    cot_any,
    gate_any,
    gate_far,
    up_any,
    up_far,
    down_any,
    wo_any,
    wo_far,
    out_ref,
    d_res_ref,
    grad_ref,
    d_gain_ref,
    d_gate_ref,
    d_up_ref,
    d_down_ref,
    d_wo_ref,
    gate,
    up,
    down,
    wo,
    cot,
    land,
    d_hidden,
    hidden,
    d_gate,
    d_up,
    sum_send,
    sum_land,
    out_send,
    out_land,
    d_down,
    res_own,
    res_land,
    swap_own,
    load_sem,
    ffn_send,
    ffn_recv,
    sum_ssem,
    sum_rsem,
    out_ssem,
    out_rsem,
    res_send,
    res_recv,
    swap_send,
    swap_recv,
):
    here = place()
    outer, inner, fsdp = here
    part = ffn_ref.shape[1]
    width = ffn_ref.shape[2]
    depth = width // 2
    rows = 2 * part
    pair = 2 * rows
    reach = gate.shape[1]
    odd = inner % 2
    chip = (inner // 2) * 2 + fsdp
    my_slot = slot_of(here)
    me = member_of(here)
    lane = fsdp * 4 + inner
    tiles = 2 * (reach // BLOCK) - 1
    step = (reach // BLOCK - 1) * BLOCK
    start = pl.multiple_of((lane // 2) * tiles * BLOCK + odd * step, BLOCK)
    down_start = pl.multiple_of((inner // 2) * tiles * BLOCK + odd * step, BLOCK)
    mine_at = pl.ds(pl.multiple_of(fsdp * depth, depth), depth)
    far_at = pl.ds(pl.multiple_of((1 - fsdp) * depth, depth), depth)
    pad = BLOCK // 2

    ready = greet([group_peer(k) for k in range(1, 8)])
    loads = [
        pltpu.make_async_copy(src, dst, load_sem.at[n])
        for n, (src, dst) in enumerate(
            (
                (down_any.at[pl.ds(down_start, reach)], down),
                (cot_any, cot),
                (gate_any.at[:, pl.ds(start, reach)], gate.at[mine_at]),
                (gate_far, gate.at[far_at]),
                (up_any.at[:, pl.ds(start, reach)], up.at[mine_at]),
                (up_far, up.at[far_at]),
                (wo_any, wo.at[mine_at]),
                (wo_far, wo.at[far_at]),
            )
        )
    ]
    for copy in loads:
        copy.start()
    ready()
    gather = Gather(
        [ffn_ref],
        lambda device: [land.at[pl.ds(pl.multiple_of(slot_of(device) * 2, 2), 2)]],
        ffn_send,
        ffn_recv,
    )
    gather.start()
    land[pl.ds(pl.multiple_of(my_slot * 2, 2), 2)] = ffn_ref[...]
    loads[0].wait()
    loads[1].wait()

    def chip_rows(n):
        return pl.ds(pl.multiple_of(((chip + n) % 4) * pair, pair), pair)

    def four(n):
        return pl.ds(pl.multiple_of(((chip + n) % 4) * 4, 4), 4)

    @pl.loop(0, 4)
    def _(n):
        values = cot[four(n)].reshape(pair, width)
        d_hidden[chip_rows(n), :] = dot(values, down[...], ((1,), (1,)))

    for copy in loads[2:6]:
        copy.wait()
    col = lax.broadcasted_iota(jnp.int32, (pair, reach), 1)
    valid = (col >= odd * pad) & (col < reach - pad + odd * pad)

    def outgoing(n, core):
        device_chip = (chip + n) % 4
        return (outer, (device_chip // 2) * 2 + core, device_chip % 2)

    def send_rows(n, src, dst, ssem, rsem):
        for flip in range(2):
            core = (odd + flip) % 2
            device = outgoing(n, core)
            slot = slot_of(device)
            copy = remote(src.at[slot], dst.at[my_slot], ssem.at[slot], rsem.at[my_slot], device)
            if flip:
                copy.start()
            else:
                pl.when(n > 0)(copy.start)

    @pl.loop(0, 4)
    def _(n):
        @pl.when(n > 0)
        def _():
            gather.pass_on(n)

        gather.wait(chip_peer(n, 1))
        at = chip_rows(n)
        values = land[four(n)].reshape(pair, width)
        gate_pre = dot(values, gate[...])
        up_pre = dot(values, up[...])
        sigmoid = jax.nn.sigmoid(gate_pre)
        silu = gate_pre * sigmoid
        hidden[at, :] = jnp.where(valid, silu * up_pre, 0.0).astype(BF16)
        back = jnp.where(valid, d_hidden[at, :], 0.0)
        d_gate[at, :] = (back * up_pre * sigmoid * (1.0 + gate_pre * (1.0 - sigmoid))).astype(BF16)
        d_up[at, :] = (back * silu).astype(BF16)
        total = dot(d_gate[at, :], gate[...], ((1,), (1,)))
        total = total + dot(d_up[at, :], up[...], ((1,), (1,)))
        slots = pl.ds(pl.multiple_of(((chip + n) % 4) * 2, 2), 2)
        sum_send[slots] = total.reshape(2, rows, width).astype(BF16)
        send_rows(n, sum_send, sum_land, sum_ssem, sum_rsem)

    @pl.loop(0, 4)
    def _(n):
        total = dot(hidden[chip_rows(n), :], down[...])
        slots = pl.ds(pl.multiple_of(((chip + n) % 4) * 2, 2), 2)
        out_send[slots] = total.reshape(2, rows, width).astype(BF16)
        send_rows(n, out_send, out_land, out_ssem, out_rsem)

    def receive(src, land_ref, ssem, rsem):
        total = src[my_slot].astype(F32)
        for k in range(1, 8):
            device = group_peer(k)
            slot = slot_of(device)
            remote(
                src.at[slot], land_ref.at[slot], ssem.at[slot], rsem.at[slot], device
            ).wait_recv()
            total = total + land_ref[slot].astype(F32)
        return total

    def weight_tile(left, right, ref, tile, per):
        at = pl.ds(pl.multiple_of(tile * BLOCK, BLOCK), BLOCK)
        value = dot(left[:, at], right[...], ((0,), (0,)))
        count = BLOCK // per
        ref[pl.ds(tile * count, count)] = value.reshape(count, per, reach).astype(BF16)

    cot_rows = cot.reshape(8 * rows, width)
    land_rows = land.reshape(8 * rows, width)

    @pl.loop(0, reach // BLOCK)
    def _(tile):
        at = pl.ds(pl.multiple_of(tile * BLOCK, BLOCK), BLOCK)
        d_down[at, :] = dot(hidden[:, at], cot_rows[...], ((0,), (0,)))

    for copy in loads[6:]:
        copy.wait()
    error = receive(sum_send, sum_land, sum_ssem, sum_rsem)
    residual = residual_ref[...].reshape(rows, width)
    inverse = lax.rsqrt(jnp.mean(residual * residual, axis=-1, keepdims=True) + EPS)
    scaled = error * gain_ref[...]
    inner_mean = jnp.mean(scaled * residual, axis=-1, keepdims=True)
    back = inverse * scaled - residual * (inverse * inverse * inverse) * inner_mean
    d_gain_ref[...] = jnp.sum(error * residual * inverse, axis=0, keepdims=True)
    d_residual = dy_ref[...].reshape(rows, width).astype(F32) + back
    d_res_ref[...] = d_residual.reshape(2, part, width)
    res_own[...] = d_residual.astype(BF16).reshape(2, part, width)
    attn_grad = dot(d_residual.astype(BF16), wo[...], ((1,), (1,)))
    swap_own[...] = attn_grad.astype(BF16).reshape(2, part, width)

    def head_cols(device):
        source = device[2] * 4 + device[1]
        return pl.ds(pl.multiple_of(source * 2 * HEAD, 2 * HEAD), 2 * HEAD)

    def token_at(ref, device):
        member = member_of(device)
        return [
            ref.at[0, pl.ds(early_row(member, part), part)],
            ref.at[1, pl.ds(late_row(member, part), part)],
        ]

    def swap_copy(k, n, owner):
        device = group_peer(k)
        return remote(
            swap_own.at[n, :, head_cols(device)],
            token_at(grad_ref, owner)[n],
            swap_send.at[n, k],
            swap_recv.at[n, slot_of(owner)],
            device,
        )

    for k in range(1, 8):
        for n in range(2):
            swap_copy(k, n, here).start()
    wide = Gather(
        [res_own.at[0], res_own.at[1]],
        lambda device: token_at(res_land, device),
        res_send,
        res_recv,
    )
    wide.start()
    grad_ref[0, pl.ds(early_row(me, part), part)] = swap_own[0, :, head_cols(here)]
    grad_ref[1, pl.ds(late_row(me, part), part)] = swap_own[1, :, head_cols(here)]
    res_land[0, pl.ds(early_row(me, part), part)] = res_own[0]
    res_land[1, pl.ds(late_row(me, part), part)] = res_own[1]

    per = d_gate_ref.shape[1]

    @pl.loop(0, width // BLOCK)
    def _(tile):
        weight_tile(land_rows, d_gate, d_gate_ref, tile, per)
        weight_tile(land_rows, d_up, d_up_ref, tile, per)

    for k in (1, 3, 2):
        wide.pass_on(k)
    total = receive(out_send, out_land, out_ssem, out_rsem)
    out_ref[...] = (total + residual_ref[...].reshape(rows, width)).reshape(
        2, part, width
    ).astype(BF16)

    down_per = d_down_ref.shape[1]

    for z in range(steps):
        at = z * down_per
        even_rows = d_down[at : at + down_per, :]
        odd_rows = d_down[at + pad : at + pad + down_per, :]
        d_down_ref[z] = jnp.where(odd > 0, odd_rows, even_rows).astype(BF16)

    wide.finish()
    half = res_land.shape[1]
    value = dot(
        attn_ref[...].reshape(2 * half, 2 * HEAD),
        res_land[...].reshape(2 * half, width),
        ((0,), (0,)),
    )
    d_wo_ref[...] = value.reshape(d_wo_ref.shape).astype(BF16)
    for k in range(1, 8):
        device = group_peer(k)
        for n in range(2):
            swap_copy(k, n, device).wait_recv()
            swap_copy(k, n, here).wait_send()
        slot = slot_of(device)
        remote(
            sum_send.at[slot], sum_land.at[slot], sum_ssem.at[slot], sum_rsem.at[slot], device
        ).wait_send()
        remote(
            out_send.at[slot], out_land.at[slot], out_ssem.at[slot], out_rsem.at[slot], device
        ).wait_send()
    gather.drain()
    wide.drain()


def ffn(ffn_rows, residual, dy, attn, gain, cot, weights, steps, devices):
    part, width = ffn_rows.shape[1:]
    gate, gate_far, up, up_far, down, wo, wo_far = weights
    reach = gate_far.shape[1]
    own_ff = reach - BLOCK // 2
    rows = 2 * part
    half = attn.shape[1]
    tokens = 2 * half
    block = pltpu.VMEM((8, rows, width), BF16)
    return pl.pallas_call(
        functools.partial(ffn_kernel, steps),
        out_shape=(
            jax.ShapeDtypeStruct((2, part, width), BF16),
            jax.ShapeDtypeStruct((2, part, width), F32),
            jax.ShapeDtypeStruct((2, half, 2 * HEAD), BF16),
            jax.ShapeDtypeStruct((1, width), F32),
            jax.ShapeDtypeStruct((devices, width // devices, reach), BF16),
            jax.ShapeDtypeStruct((devices, width // devices, reach), BF16),
            jax.ShapeDtypeStruct((steps, own_ff // steps, width), BF16),
            jax.ShapeDtypeStruct((steps, 2 * HEAD // steps, width), BF16),
        ),
        in_specs=[VMEM] * 5 + [ANY] * 8,
        out_specs=[VMEM] * 8,
        scratch_shapes=[
            pltpu.VMEM((width, reach), BF16),
            pltpu.VMEM((width, reach), BF16),
            pltpu.VMEM((reach, width), BF16),
            pltpu.VMEM((width, width), BF16),
            pltpu.VMEM((16, part, width), BF16),
            pltpu.VMEM((16, part, width), BF16),
            pltpu.VMEM((tokens, reach), F32),
            pltpu.VMEM((tokens, reach), BF16),
            pltpu.VMEM((tokens, reach), BF16),
            pltpu.VMEM((tokens, reach), BF16),
            block,
            block,
            block,
            block,
            pltpu.VMEM((reach, width), F32),
            pltpu.VMEM((2, part, width), BF16),
            pltpu.VMEM((2, half, width), BF16),
            pltpu.VMEM((2, part, width), BF16),
            DMA((8,)),
            DMA((1, 8)),
            DMA((1, 8)),
            DMA((8,)),
            DMA((8,)),
            DMA((8,)),
            DMA((8,)),
            DMA((2, 8)),
            DMA((2, 8)),
            DMA((2, 8)),
            DMA((2, 8)),
        ],
        compiler_params=params(2),
        name="ffn",
    )(ffn_rows, residual, dy, attn, gain, cot, gate, gate_far, up, up_far, down, wo, wo_far)


def member_device(number):
    return (number // 8, number % 8 // 2, number % 2)


def number_of(device):
    return device[0] * 8 + device[1] * 2 + device[2]


def lane_of(device):
    return device[2] * 4 + device[1]


def lane_device(outer, lane):
    return (outer, lane % 4, lane // 4)


def back_kernel(
    steps,
    qt_ref,
    q_ref,
    grad_ref,
    attn_t_ref,
    log_ref,
    kv_ref,
    proj_ref,
    cos_ref,
    sin_ref,
    qg_ref,
    kg_ref,
    x_ref,
    d_res_ref,
    gain_ref,
    ffn_gain_ref,
    normed_any,
    weights_any,
    far_any,
    d_gate_any,
    d_up_any,
    d_down_any,
    d_wo_any,
    dx_ref,
    gains_ref,
    own_q_ref,
    own_k_ref,
    own_v_ref,
    own_o_ref,
    own_gate_ref,
    own_up_ref,
    own_down_ref,
    normed,
    weights,
    far,
    gt_ref,
    g_ref,
    delta_ref,
    acc_ref,
    dkv_ref,
    dkv_send,
    dkv_land,
    d_qkv,
    tokens_land,
    d_weights,
    gate_land,
    up_land,
    qkv_land,
    down_land,
    wo_land,
    sums,
    sums_land,
    load_sem,
    gate_send,
    gate_recv,
    up_send,
    up_recv,
    qkv_send,
    qkv_recv,
    down_send,
    down_recv,
    wo_send,
    wo_recv,
    kv_send,
    kv_recv,
    swap_send,
    swap_recv,
    near_send,
    near_recv,
    far_send,
    far_recv,
):
    here = place()
    outer, inner, fsdp = here
    lane = lane_of(here)
    number = number_of(here)
    me = member_of(here)
    count = steps * 8
    part, width = x_ref.shape[1:]
    rows = 2 * part
    half = normed.shape[1]
    sub = half // 2
    wide = 2 * sub
    depth = width // 2

    barrier = pltpu.get_barrier_semaphore()

    @pl.loop(1, count)
    def _(k):
        pl.semaphore_signal(
            barrier,
            inc=1,
            device_id=member_device((number + k) % count),
            device_id_type=pl.DeviceIdType.MESH,
        )

    loads = [
        pltpu.make_async_copy(src, dst, load_sem.at[n])
        for n, (src, dst) in enumerate(
            ((normed_any, normed), (weights_any, weights), (far_any, far))
        )
    ]
    for copy in loads:
        copy.start()
    acc_ref[...] = jnp.zeros_like(acc_ref)
    dkv_ref[...] = jnp.zeros_like(dkv_ref)
    low = lax.broadcasted_iota(jnp.int32, (sub, 2 * HEAD), 1) < HEAD
    front = lax.broadcasted_iota(jnp.int32, (sub, 2 * HEAD), 1) % HEAD < HEAD // 2

    @pl.loop(0, 4)
    def _(tile):
        inside = pl.ds(pl.multiple_of((tile % 2) * sub, sub), sub)
        values = grad_ref[tile // 2, inside, :].astype(F32)
        flipped = pltpu.roll(values, HEAD, 1)
        for head, shifted in enumerate((flipped, values)):
            cols = pl.ds(pl.multiple_of(tile * wide + head * sub, sub), sub)
            shifted = jnp.where(low, 0.0, shifted)
            turned = shifted.T
            g_ref[cols, :] = shifted.astype(BF16)
            gt_ref[:, cols] = turned.astype(BF16)
            delta_ref[:, cols] = jnp.sum(
                turned[HEAD:] * attn_t_ref[:, cols], axis=0, keepdims=True
            )

    pl.semaphore_wait(barrier, count - 1)

    def rows_copy(src, land, ssem, rsem, target, source):
        key = lane_of(source) * steps + source[0]
        owner = number_of(target)
        return remote(src.at[owner], land.at[key], ssem.at[owner], rsem.at[key], target)

    def slice_copy(src, land, ssem, rsem, chunk, source):
        target = member_device(lane * steps + chunk)
        return remote(src.at[chunk], land.at[source], ssem.at[chunk], rsem.at[source], target)

    slices = (
        (d_down_any, down_land, down_send, down_recv),
        (d_wo_any, wo_land, wo_send, wo_recv),
    )
    mine = number // steps == lane

    @pl.loop(0, steps)
    def _(k):
        chunk = (outer + k) % steps
        away = lane * steps + chunk != number

        @pl.when(away)
        def _():
            for refs in slices:
                slice_copy(*refs, chunk, outer).start()

    @pl.when(mine)
    def _():
        for n, (src, land, _, _) in enumerate(slices):
            copy = pltpu.make_async_copy(
                src.at[number % steps], land.at[outer], load_sem.at[3 + n]
            )
            copy.start()
            copy.wait()

    def outer_peer(k):
        return ((outer + k) % steps, inner, fsdp)

    def block(slot, row, size, col, mask):
        at = pl.ds(pl.multiple_of(row, sub), size)
        kv = kv_ref[slot, at, :]
        cols = pl.ds(pl.multiple_of(col, wide), wide)
        probs = jnp.exp2(dot(kv, qt_ref[:, cols]) * SCORE2 - log_ref[:, cols])
        if mask is not None:
            probs = jnp.where(mask, probs, 0.0)
        grads = dot(kv, gt_ref[:, cols])
        grads = (probs * (grads - delta_ref[:, cols]) * SCORE).astype(BF16)
        dkv_ref[slot, at, :] += dot(grads, q_ref[cols, :]) + dot(
            probs.astype(BF16), g_ref[cols, :]
        )
        acc_ref[:, cols] += dot(kv, grads, ((0,), (0,)))

    def kv_copy(slot, late, source):
        at = pl.ds(late * half, half)
        return remote(
            dkv_send.at[slot, at],
            dkv_land.at[source, at],
            kv_send.at[late, slot],
            kv_recv.at[late, source],
            (slot, inner, fsdp),
        )

    @pl.loop(1, steps)
    def _(k):
        slot = (outer + k) % steps
        late = jnp.where(slot < outer, 0, 1)

        @pl.loop(0, 2)
        def _(n):
            block(slot, 0, half, (2 + n) * wide, None)
            block(slot, late * half, half, (late * 2 + n) * wide, None)

        dkv_send[slot] = dkv_ref[slot].astype(BF16)
        kv_copy(slot, 0, outer).start()

        @pl.when(slot > outer)
        def _():
            kv_copy(slot, 1, outer).start()

    key = lax.broadcasted_iota(jnp.int32, (sub, wide), 0)
    query = lax.broadcasted_iota(jnp.int32, (sub, wide), 1) % sub
    diagonal = key <= query

    @pl.loop(0, 2)
    def _(late):
        block(outer, late * half, sub, late * 2 * wide, diagonal)
        block(outer, late * half, sub, late * 2 * wide + wide, None)
        block(outer, late * half + sub, sub, late * 2 * wide + wide, diagonal)

    @pl.loop(0, 2)
    def _(n):
        block(outer, 0, half, (2 + n) * wide, None)

    def rope_back(grads, at):
        return grads * cos_ref[at, :] + halves(grads * sin_ref[at, :], front)

    def norm_back(raw, grads, gain):
        inverse = head_inverse(raw, low)
        scaled = grads * gain
        product = scaled * raw
        first = jnp.sum(jnp.where(low, product, 0.0), axis=-1, keepdims=True)
        second = jnp.sum(jnp.where(low, 0.0, product), axis=-1, keepdims=True)
        inner_mean = jnp.where(low, first, second) * (1.0 / HEAD)
        back = inverse * scaled - raw * (inverse * inverse * inverse) * inner_mean
        return back, jnp.sum(grads * raw * inverse, axis=0, keepdims=True)

    sums[...] = jnp.zeros_like(sums)

    @pl.loop(0, 4)
    def _(tile):
        heads = []
        for head in range(2):
            cols = pl.ds(pl.multiple_of(tile * wide + head * sub, sub), sub)
            heads.append(acc_ref[:HEAD, cols])
        at = pl.ds(pl.multiple_of(tile * sub, sub), sub)
        inside = pl.ds(pl.multiple_of((tile % 2) * sub, sub), sub)
        grads = rope_back(jnp.concatenate(heads, axis=0).T, at)
        back, gain = norm_back(proj_ref[at, : 2 * HEAD], grads, qg_ref[...])
        d_qkv[tile // 2, inside, : 2 * HEAD] = back.astype(BF16)
        sums[2:3, : 2 * HEAD] += gain

    @pl.loop(1, steps)
    def _(k):
        source = (outer + k) % steps
        kv_copy(source, 0, source).wait_recv()
        early = pl.ds(0, half)
        dkv_ref[outer, early, :] += dkv_land[source, early, :].astype(F32)

        @pl.when(source < outer)
        def _():
            kv_copy(source, 1, source).wait_recv()
            at = pl.ds(half, half)
            dkv_ref[outer, at, :] += dkv_land[source, at, :].astype(F32)

    @pl.loop(1, count)
    def _(k):
        target = member_device((number + k) % count)
        rows_copy(d_gate_any, gate_land, gate_send, gate_recv, target, here).start()
        rows_copy(d_up_any, up_land, up_send, up_recv, target, here).start()

    own_key = lane * steps + outer
    own_rows = [
        pltpu.make_async_copy(src.at[number], land.at[own_key], load_sem.at[n])
        for n, (src, land) in ((3, (d_gate_any, gate_land)), (4, (d_up_any, up_land)))
    ]
    for copy in own_rows:
        copy.start()

    @pl.loop(0, 4)
    def _(tile):
        at = pl.ds(pl.multiple_of(tile * sub, sub), sub)
        inside = pl.ds(pl.multiple_of((tile % 2) * sub, sub), sub)
        grads = dkv_ref[outer, at, :]
        raw = proj_ref[at, 2 * HEAD :]
        back, gain = norm_back(raw, jnp.where(low, rope_back(grads, at), 0.0), kg_ref[...])
        d_qkv[tile // 2, inside, 2 * HEAD :] = jnp.where(low, back, grads).astype(BF16)
        sums[2:3, 2 * HEAD : 4 * HEAD] += gain

    def token_at(ref, device):
        member = member_of(device)
        return [
            ref.at[0, pl.ds(early_row(member, part), part)],
            ref.at[1, pl.ds(late_row(member, part), part)],
        ]

    def lane_cols(device):
        return pl.ds(pl.multiple_of(lane_of(device) * 4 * HEAD, 4 * HEAD), 4 * HEAD)

    def swap_copy(k, n, owner):
        device = group_peer(k)
        return remote(
            token_at(d_qkv, device)[n],
            tokens_land.at[n, :, lane_cols(owner)],
            swap_send.at[n, k],
            swap_recv.at[n, slot_of(owner)],
            device,
        )

    for k in range(1, 8):
        for n in range(2):
            swap_copy(k, n, here).start()
    tokens_land[0, :, lane_cols(here)] = d_qkv[0, pl.ds(early_row(me, part), part), :]
    tokens_land[1, :, lane_cols(here)] = d_qkv[1, pl.ds(late_row(me, part), part), :]

    for copy in loads:
        copy.wait()
    per = d_weights.shape[1]
    normed_rows = normed.reshape(2 * half, width)
    d_rows = d_qkv.reshape(2 * half, 4 * HEAD)

    @pl.loop(0, width // BLOCK)
    def _(tile):
        at = pl.ds(pl.multiple_of(tile * BLOCK, BLOCK), BLOCK)
        value = dot(normed_rows[:, at], d_rows[...], ((0,), (0,)))
        many = BLOCK // per
        d_weights[pl.ds(tile * many, many)] = value.reshape(many, per, 4 * HEAD).astype(BF16)

    @pl.loop(1, count)
    def _(k):
        target = member_device((number + k) % count)
        rows_copy(d_weights, qkv_land, qkv_send, qkv_recv, target, here).start()

    qkv_land[own_key] = d_weights[number]

    for k in range(1, 8):
        for n in range(2):
            swap_copy(k, n, group_peer(k)).wait_recv()
    mine_at = pl.ds(pl.multiple_of(fsdp * depth, depth), depth)
    far_at = pl.ds(pl.multiple_of((1 - fsdp) * depth, depth), depth)
    grads = tokens_land[...].reshape(rows, 8 * 4 * HEAD)
    flat = dx_ref.reshape(rows, width)
    flat[:, mine_at] = dot(grads, weights[...], ((1,), (1,)))
    flat[:, far_at] = dot(grads, far[...], ((1,), (1,)))
    error = flat[...]
    inputs = x_ref[...].reshape(rows, width).astype(F32)
    inverse = lax.rsqrt(jnp.mean(inputs * inputs, axis=-1, keepdims=True) + EPS)
    scaled = error * gain_ref[...]
    inner_mean = jnp.mean(scaled * inputs, axis=-1, keepdims=True)
    back = inverse * scaled - inputs * (inverse * inverse * inverse) * inner_mean
    flat[...] = d_res_ref[...].reshape(rows, width) + back
    sums[0:1, :] = jnp.sum(error * inputs * inverse, axis=0, keepdims=True)
    sums[1:2, :] = ffn_gain_ref[...]

    def near_copy(k, owner):
        return remote(
            sums, sums_land.at[slot_of(owner)], near_send.at[k], near_recv.at[slot_of(owner)],
            group_peer(k),
        )

    def far_copy(k, owner):
        return remote(
            gains_ref, sums_land.at[8 + owner], far_send.at[k], far_recv.at[owner], outer_peer(k)
        )

    for k in range(1, 8):
        near_copy(k, here).start()
    total = sums[...]
    for k in range(1, 8):
        near_copy(k, group_peer(k)).wait_recv()
        total = total + sums_land[slot_of(group_peer(k))]
    gains_ref[...] = total

    @pl.loop(1, steps)
    def _(k):
        far_copy(k, outer).start()

    @pl.loop(0, steps)
    def _(z):
        source = lane_device(z, number // steps)

        @pl.when(number_of(source) != number)
        def _():
            for src, land, ssem, rsem in slices:
                remote(
                    src.at[0], land.at[z], ssem.at[0], rsem.at[z], here
                ).wait_recv()

    own_down_ref[...] = jnp.zeros_like(own_down_ref)
    own_o_ref[...] = jnp.zeros_like(own_o_ref)

    @pl.loop(0, steps)
    def _(z):
        own_down_ref[...] += down_land[z].astype(F32)
        own_o_ref[...] += wo_land[z].astype(F32)

    for copy in own_rows:
        copy.wait()

    @pl.loop(1, count)
    def _(k):
        source = member_device((number + k) % count)
        rows_copy(d_gate_any, gate_land, gate_send, gate_recv, here, source).wait_recv()
        rows_copy(d_up_any, up_land, up_send, up_recv, here, source).wait_recv()
        rows_copy(d_weights, qkv_land, qkv_send, qkv_recv, here, source).wait_recv()

    def added(land, which):
        total = land[which * steps].astype(F32)
        for z in range(1, steps):
            total = total + land[which * steps + z].astype(F32)
        return total

    reach = gate_land.shape[2]
    tiles = 2 * (reach // BLOCK) - 1
    step = reach - BLOCK
    for pair in range(4):
        base = pair * tiles * BLOCK
        for land, ref in ((gate_land, own_gate_ref), (up_land, own_up_ref)):
            first, second = added(land, 2 * pair), added(land, 2 * pair + 1)
            ref[:, base : base + step] = first[:, :step]
            ref[:, base + step : base + reach] = first[:, step:] + second[:, :BLOCK]
            ref[:, base + reach : base + tiles * BLOCK] = second[:, BLOCK:]
        first, second = added(qkv_land, 2 * pair), added(qkv_land, 2 * pair + 1)
        twice = 2 * HEAD
        own_q_ref[:, 2 * pair * twice : (2 * pair + 1) * twice] = first[:, :twice]
        own_q_ref[:, (2 * pair + 1) * twice : (2 * pair + 2) * twice] = second[:, :twice]
        first, second = first[:, twice:], second[:, twice:]
        lower = lax.broadcasted_iota(jnp.int32, first.shape, 1) < HEAD
        at = slice(pair * twice, (pair + 1) * twice)
        own_k_ref[:, at] = jnp.where(lower, first, pltpu.roll(second, HEAD, 1))
        own_v_ref[:, at] = jnp.where(lower, pltpu.roll(first, HEAD, 1), second)

    @pl.loop(1, steps)
    def _(k):
        far_copy(k, outer).wait_send()

    total = gains_ref[...]

    @pl.loop(1, steps)
    def _(k):
        source = (outer + k) % steps
        far_copy(k, source).wait_recv()
        gains_ref[...] += sums_land[8 + source]

    for k in range(1, 8):
        near_copy(k, here).wait_send()
        for n in range(2):
            swap_copy(k, n, here).wait_send()

    @pl.loop(0, steps)
    def _(chunk):
        @pl.when(lane * steps + chunk != number)
        def _():
            for refs in slices:
                slice_copy(*refs, chunk, outer).wait_send()

    @pl.loop(1, steps)
    def _(k):
        slot = (outer + k) % steps
        kv_copy(slot, 0, outer).wait_send()

        @pl.when(slot > outer)
        def _():
            kv_copy(slot, 1, outer).wait_send()

    @pl.loop(1, count)
    def _(k):
        target = member_device((number + k) % count)
        rows_copy(d_gate_any, gate_land, gate_send, gate_recv, target, here).wait_send()
        rows_copy(d_up_any, up_land, up_send, up_recv, target, here).wait_send()
        rows_copy(d_weights, qkv_land, qkv_send, qkv_recv, target, here).wait_send()


def back(args, steps):
    q_t, q_cols = args[0], args[1]
    kv, x = args[5], args[11]
    normed, weights = args[15], args[16]
    d_gate, d_down, d_wo = args[18], args[20], args[21]
    part, width = x.shape[1:]
    half = normed.shape[1]
    tokens = 2 * half
    count = steps * 8
    per = width // count
    reach = d_gate.shape[2]
    ff = (2 * (reach // BLOCK) - 1) * BLOCK * 4
    own = lambda *shape: jax.ShapeDtypeStruct(shape, F32)
    kv_cols = 8 * HEAD
    return pl.pallas_call(
        functools.partial(back_kernel, steps),
        out_shape=(
            own(2, part, width),
            own(8, width),
            own(per, 16 * HEAD),
            own(per, kv_cols),
            own(per, kv_cols),
            own(*d_wo.shape[1:]),
            own(per, ff),
            own(per, ff),
            own(*d_down.shape[1:]),
        ),
        in_specs=[VMEM] * 15 + [ANY] * 7,
        out_specs=[VMEM] * 9,
        scratch_shapes=[
            pltpu.VMEM(normed.shape, BF16),
            pltpu.VMEM(weights.shape, BF16),
            pltpu.VMEM(weights.shape, BF16),
            pltpu.VMEM(q_t.shape, BF16),
            pltpu.VMEM(q_cols.shape, BF16),
            pltpu.VMEM((1, 2 * tokens), F32),
            pltpu.VMEM(q_t.shape, F32),
            pltpu.VMEM(kv.shape, F32),
            pltpu.VMEM(kv.shape, BF16),
            pltpu.VMEM(kv.shape, BF16),
            pltpu.VMEM((2, half, 4 * HEAD), BF16),
            pltpu.VMEM((2, part, 32 * HEAD), BF16),
            pltpu.VMEM((count, per, 4 * HEAD), BF16),
            pltpu.VMEM((count, per, reach), BF16),
            pltpu.VMEM((count, per, reach), BF16),
            pltpu.VMEM((count, per, 4 * HEAD), BF16),
            pltpu.VMEM(d_down.shape, BF16),
            pltpu.VMEM(d_wo.shape, BF16),
            pltpu.VMEM((8, width), F32),
            pltpu.VMEM((8 + steps, 8, width), F32),
            DMA((5,)),
            DMA((count,)),
            DMA((count,)),
            DMA((count,)),
            DMA((count,)),
            DMA((count,)),
            DMA((count,)),
            DMA((steps,)),
            DMA((steps,)),
            DMA((steps,)),
            DMA((steps,)),
            DMA((2, steps)),
            DMA((2, steps)),
            DMA((2, 8)),
            DMA((2, 8)),
            DMA((8,)),
            DMA((8,)),
            DMA((steps,)),
            DMA((steps,)),
        ],
        compiler_params=params(3),
        name="back",
    )(*args)


def swap(array, axis_size):
    return lax.ppermute(array, "fsdp", [(k, (k + 1) % axis_size) for k in range(axis_size)])


def local(
    block_input, dy, attn_gain, q_gain, k_gain, ffn_gain, wq, wk, wv, wo, w_gate, w_up, w_down
):
    steps = lax.axis_size("outer")
    inner_size = lax.axis_size("inner")
    fsdp_size = lax.axis_size("fsdp")
    outer = lax.axis_index("outer")
    inner = lax.axis_index("inner")
    fsdp = lax.axis_index("fsdp")
    group = inner_size * fsdp_size
    part, width = block_input.shape[2:]
    half = inner_size * fsdp_size * part
    ff = w_gate.shape[1]
    tiles = 2 * ff // group // BLOCK
    reach = (tiles + 1) // 2 * BLOCK
    far_lane = (1 - fsdp) * inner_size + inner
    far_start = (far_lane // 2 * tiles + inner % 2 * (tiles // 2)) * BLOCK

    def window(arr, start, size):
        return lax.dynamic_slice_in_dim(arr, start, size, 1)

    depth = wq.shape[0]
    weights = jnp.concatenate(
        [
            wq.reshape(depth, group, 2 * HEAD),
            wk.reshape(depth, group, HEAD),
            wv.reshape(depth, group, HEAD),
        ],
        axis=2,
    ).reshape(depth, group * 4 * HEAD)
    qkv_far = swap(window(weights, far_lane * 4 * HEAD, 4 * HEAD), fsdp_size)
    wo_far = swap(wo, fsdp_size)
    gate_far = swap(window(w_gate, far_start, reach), fsdp_size)
    up_far = swap(window(w_up, far_start, reach), fsdp_size)

    x = block_input.reshape(2, part, width)
    cot = dy.reshape(2, part, width)
    within = jnp.arange(half, dtype=jnp.int32)
    positions = jnp.concatenate(
        [outer * half + within, (2 * steps - 1 - outer) * half + within], axis=0
    )
    index = jnp.arange(2 * HEAD, dtype=jnp.int32) % (HEAD // 2)
    frequency = ROPE_BASE ** (-2.0 * index.astype(F32) / HEAD)
    angles = positions.astype(F32)[:, None] * frequency[None, :]
    sign = jnp.where(jnp.arange(2 * HEAD) % HEAD < HEAD // 2, -1.0, 1.0).astype(F32)
    cos = jnp.cos(angles)
    sin = jnp.sin(angles) * sign
    q_gain2 = jnp.tile(q_gain, 2)[None]
    k_gain2 = jnp.tile(k_gain, 2)[None]
    normed, proj, q_cols, q_t, kv_own = front(
        x, attn_gain[None], weights, qkv_far, cos, sin, q_gain2, k_gain2
    )
    kv, cot_group, attn_t, log_total, attn, residual, ffn_rows = middle(
        x, cot, q_t, kv_own, wo, wo_far, ffn_gain[None], steps
    )
    later, ffn_rows = lax.optimization_barrier((weights, ffn_rows))
    weights_far = swap(later, fsdp_size)
    result, d_residual, attn_grad, d_ffn_gain, d_gate, d_up, d_down, d_wo = ffn(
        ffn_rows,
        residual,
        cot,
        attn,
        ffn_gain[None],
        cot_group.reshape(2 * group, part, width),
        (w_gate, gate_far, w_up, up_far, w_down, wo, wo_far),
        steps,
        steps * group,
    )
    grad_in, gains, own_q, own_k, own_v, own_o, own_gate, own_up, own_down = back(
        (
            q_t,
            q_cols,
            attn_grad,
            attn_t,
            log_total,
            kv,
            proj,
            cos,
            sin,
            q_gain2,
            k_gain2,
            x,
            d_residual,
            attn_gain[None],
            d_ffn_gain,
            normed,
            weights,
            weights_far,
            d_gate,
            d_up,
            d_down,
            d_wo,
        ),
        steps,
    )
    return (
        result.reshape(block_input.shape),
        grad_in.reshape(block_input.shape),
        gains[0],
        gains[2, :HEAD] + gains[2, HEAD : 2 * HEAD],
        gains[2, 2 * HEAD : 3 * HEAD],
        gains[1],
        own_q,
        own_k,
        own_v,
        own_o,
        own_gate,
        own_up,
        own_down,
    )


def solution(mesh):
    ctx, fsdp = mesh.shape["ctx"], mesh.shape["fsdp"]
    inner = 8 // fsdp
    grid = Mesh(mesh.devices.reshape(ctx // inner, inner, fsdp), EVERY)
    tokens = P(None, ("outer", "inner"), "fsdp", None)
    shard = P("fsdp", None)
    owned = P(EVERY, None)
    return jax.shard_map(
        local,
        mesh=grid,
        in_specs=(tokens, tokens) + (P(),) * 4 + (shard,) * 7,
        out_specs=(tokens, tokens) + (P(),) * 4 + (owned,) * 7,
        check_vma=False,
    )
```

```python
import functools
import math

import jax
import jax.numpy as jnp
from jax import lax
from jax.experimental import pallas as pl
from jax.experimental.pallas import tpu as pltpu
from jax.sharding import Mesh
from jax.sharding import PartitionSpec as P

EPS = 1e-05
ROPE_BASE = 1000000.0
F32 = jnp.float32
BF16 = jnp.bfloat16
HEAD = 64
BLOCK = 128
GROUP = ("inner", "fsdp")
EVERY = ("outer", "inner", "fsdp")


def dot(a, b, dims=((1,), (0,))):
    return lax.dot_general(a, b, (dims, ((), ())), preferred_element_type=F32)


SCORE = 1.0 / math.sqrt(HEAD)
SCORE2 = SCORE * math.log2(math.e)


def place():
    return tuple(lax.axis_index(name) for name in EVERY)


def remote(src, dst, send, recv, device):
    return pltpu.make_async_remote_copy(
        src_ref=src,
        dst_ref=dst,
        send_sem=send,
        recv_sem=recv,
        device_id=device,
        device_id_type=pl.DeviceIdType.MESH,
    )


def greet(devices):
    barrier = pltpu.get_barrier_semaphore()
    for device in devices:
        pl.semaphore_signal(
            barrier, inc=1, device_id=device, device_id_type=pl.DeviceIdType.MESH
        )
    return lambda: pl.semaphore_wait(barrier, len(devices))


def chip_peer(n, other_core=0):
    outer, inner, fsdp = place()
    row = (inner // 2 + n // 2) % 2
    return (outer, row * 2 + (inner + other_core) % 2, (fsdp + n) % 2)


def sibling():
    return chip_peer(0, 1)


def group_peer(k):
    outer, inner, fsdp = place()
    member = (inner * 2 + fsdp + k) % 8
    return (outer, member // 2, member % 2)


def member_of(device):
    return device[1] * 2 + device[2]


def slot_of(device):
    return ((device[1] // 2) * 2 + device[2]) * 2 + device[1] % 2


def member_device(number):
    return (number // 8, number % 8 // 2, number % 2)


def number_of(device):
    return device[0] * 8 + device[1] * 2 + device[2]


def lane_of(device):
    return device[2] * 4 + device[1]


def early_row(member, part):
    return pl.multiple_of(member * part, part)


def late_row(member, part):
    return pl.multiple_of((3 - member // 2) * 2 * part + (member % 2) * part, part)


def token_at(ref, device, part):
    member = member_of(device)
    return [
        ref.at[0, pl.ds(early_row(member, part), part)],
        ref.at[1, pl.ds(late_row(member, part), part)],
    ]


class Gather:
    def __init__(self, own, land, send, recv):
        self.own, self.land, self.send, self.recv = own, land, send, recv
        self.pieces = range(len(own))

    def copy(self, src, owner, piece, slot, device):
        return remote(
            src,
            self.land(owner)[piece],
            self.send.at[piece, slot],
            self.recv.at[piece, slot_of(owner)],
            device,
        )

    def start(self):
        for slot, device in ((1, chip_peer(1)), (2, chip_peer(2)), (0, sibling())):
            for piece in self.pieces:
                self.copy(self.own[piece], place(), piece, slot, device).start()

    def wait(self, owner):
        for piece in self.pieces:
            dst = self.land(owner)[piece]
            self.copy(dst, owner, piece, 0, sibling()).wait_recv()

    def pass_on(self, n):
        owner = chip_peer(n)
        self.wait(owner)

        def row_copies():
            for piece in self.pieces:
                self.copy(self.land(owner)[piece], owner, piece, 3, chip_peer(2)).start()

        pl.when(n == 1)(row_copies)
        for piece in self.pieces:
            self.copy(self.land(owner)[piece], owner, piece, 3 + n, sibling()).start()

    def finish(self):
        for n in range(4):
            self.wait(chip_peer(n, 1))

    def drain(self):
        for slot in range(7):
            for piece in self.pieces:
                self.copy(self.own[piece], place(), piece, slot, sibling()).wait_send()


class Exchange:
    def __init__(self, src, land, there, send, recv):
        self.src, self.land, self.there = src, land, there
        self.send, self.recv = send, recv
        self.rows = src.shape[0] // 4

    def at(self, ref, quarter):
        return ref.at[pl.ds(pl.multiple_of(quarter * self.rows, self.rows), self.rows)]

    def copy(self, src, quarter, slot, device):
        land = self.land if slot else self.there
        return remote(
            src, self.at(land, quarter), self.send.at[slot], self.recv.at[quarter], device
        )

    def start(self):
        inner = place()[1]
        self.copy(self.at(self.src, inner), inner, 0, chip_peer(1)).start()

    def shares(self):
        inner = place()[1]
        src = self.at(self.land, inner)
        peers = (chip_peer(2), chip_peer(2, 1), sibling())
        return [self.copy(src, inner, 1 + n, device) for n, device in enumerate(peers)]

    def wait(self, quarter):
        self.copy(self.at(self.land, quarter), quarter, 1, chip_peer(1)).wait_recv()

    def share(self):
        self.wait(place()[1])
        for copy in self.shares():
            copy.start()

    def finish(self):
        inner = place()[1]
        for k in range(1, 4):
            self.wait((inner + k) % 4)
        self.copy(self.at(self.src, inner), inner, 0, chip_peer(1)).wait_send()
        for copy in self.shares():
            copy.wait_send()


def rms_rows(values, gain):
    inverse = lax.rsqrt(jnp.mean(values * values, axis=-1, keepdims=True) + EPS)
    return values * inverse * gain


def head_inverse(values, low):
    squares = values * values
    first = jnp.sum(jnp.where(low, squares, 0.0), axis=-1, keepdims=True)
    second = jnp.sum(jnp.where(low, 0.0, squares), axis=-1, keepdims=True)
    return jnp.where(
        low, lax.rsqrt(first * (1.0 / HEAD) + EPS), lax.rsqrt(second * (1.0 / HEAD) + EPS)
    )


def halves(values, front):
    quarter = HEAD // 2
    return jnp.where(
        front,
        pltpu.roll(values, values.shape[-1] - quarter, 1),
        pltpu.roll(values, quarter, 1),
    )


def both(first, second, odd, flip):
    first, second = first.astype(F32), second.astype(F32)
    low = lax.broadcasted_iota(jnp.int32, first.shape, 1) < HEAD
    even = jnp.where(low, first, pltpu.roll(second, HEAD, 1))
    other = jnp.where(low, pltpu.roll(first, HEAD, 1), second)
    return jnp.where(odd > 0, other, even)


def front_kernel(
    steps,
    x_ref,
    gain_ref,
    wq_any,
    wk_any,
    wv_any,
    freq_ref,
    qg_ref,
    kg_ref,
    normed_out,
    proj_ref,
    q_ref,
    qt_ref,
    kv_ref,
    cos_ref,
    sin_ref,
    own,
    land,
    windows,
    mine_ref,
    give_ref,
    other_ref,
    send,
    recv,
    load_sem,
    far_sem,
    out_sem,
):
    outer, inner, fsdp = here = place()
    odd = inner % 2
    wide = 2 * HEAD
    loads = []
    for n, (lane, dst) in enumerate(
        ((lane_of(here), mine_ref), (lane_of(chip_peer(1)), give_ref))
    ):
        one = pl.ds(pl.multiple_of(lane * wide, wide), wide)
        two = pl.ds(pl.multiple_of(lane // 2 * wide, wide), wide)
        loads.append(
            [
                pltpu.make_async_copy(src, ref, load_sem.at[n, k])
                for k, (src, ref) in enumerate(
                    (
                        (wq_any.at[:, one], dst.at[:, pl.ds(0, wide)]),
                        (wk_any.at[:, two], windows.at[n, 0]),
                        (wv_any.at[:, two], windows.at[n, 1]),
                    )
                )
            ]
        )
    for copy in loads[1] + loads[0]:
        copy.start()
    part = x_ref.shape[1]
    half = land.shape[1]
    width = land.shape[2]
    sub = half // 2
    depth = width // 2
    ready = greet([sibling()] + [chip_peer(n) for n in (1, 2)])
    for late in range(2):
        rows = x_ref[late].astype(F32)
        own[late] = rms_rows(rows, gain_ref[...]).astype(BF16)
    for copy in loads[1]:
        copy.wait()
    give_ref[:, wide:] = both(windows[1, 0], windows[1, 1], odd, None).astype(BF16)
    ready()
    gather = Gather(
        [own.at[0], own.at[1]], lambda device: token_at(land, device, part), send, recv
    )
    gather.start()
    far = remote(give_ref, other_ref, far_sem.at[0], far_sem.at[1], chip_peer(1))
    far.start()
    me = member_of(here)
    land[0, pl.ds(early_row(me, part), part)] = own[0]
    land[1, pl.ds(late_row(me, part), part)] = own[1]
    for copy in loads[0]:
        copy.wait()
    mine_ref[:, wide:] = both(windows[0, 0], windows[0, 1], odd, None).astype(BF16)

    lane = lax.broadcasted_iota(jnp.int32, (sub, wide), 1)
    low = lane < HEAD
    front = lane % HEAD < HEAD // 2
    within = lax.broadcasted_iota(jnp.int32, (sub, wide), 0)

    @pl.loop(0, 4)
    def _(tile):
        block = jnp.where(tile < 2, outer, 2 * steps - 1 - outer)
        position = block * half + (tile % 2) * sub + within
        angle = position.astype(F32) * freq_ref[...]
        at = pl.ds(pl.multiple_of(tile * sub, sub), sub)
        sine = jnp.sin(angle)
        cos_ref[at, :] = jnp.cos(angle)
        sin_ref[at, :] = jnp.where(front, -sine, sine)

    for n in (1, 2, 3):
        gather.pass_on(n)
    gather.finish()
    out = pltpu.make_async_copy(land, normed_out, out_sem)
    out.start()
    far.wait_recv()
    mine_at = pl.ds(pl.multiple_of(fsdp * depth, depth), depth)
    other_at = pl.ds(pl.multiple_of((1 - fsdp) * depth, depth), depth)

    @pl.loop(0, 4)
    def _(tile):
        late = tile // 2
        inside = pl.ds(pl.multiple_of((tile % 2) * sub, sub), sub)
        rows = pl.ds(pl.multiple_of(tile * sub, sub), sub)
        proj = dot(land[late, inside, mine_at], mine_ref[...])
        proj = proj + dot(land[late, inside, other_at], other_ref[...])
        proj_ref[rows, :] = proj
        cos, sin = cos_ref[rows, :], sin_ref[rows, :]
        raw = proj[:, :wide]
        normed = raw * head_inverse(raw, low) * qg_ref[...]
        rotated = normed * cos + halves(normed, front) * sin
        second = pltpu.roll(rotated, HEAD, 1)
        for head, values in enumerate((rotated, second)):
            values = jnp.where(low, values, 0.0)
            cols = pl.ds(pl.multiple_of(tile * 2 * sub + head * sub, sub), sub)
            q_ref[cols, :] = values.astype(BF16)
            qt_ref[:, cols] = values.T.astype(BF16)
        raw = proj[:, wide:]
        normed = raw * head_inverse(raw, low) * kg_ref[...]
        rotated = normed * cos + halves(normed, front) * sin
        kv_ref[rows, :] = jnp.where(low, rotated, raw).astype(BF16)

    gather.drain()
    far.wait_send()
    out.wait()


def middle_kernel(
    steps,
    x_ref,
    dy_ref,
    qt_ref,
    kv_ref,
    gain_ref,
    wo_any,
    gate_any,
    up_any,
    kv_out,
    cot_out,
    wo_far,
    gate_far,
    up_far,
    attn_t_ref,
    log_ref,
    attn_ref,
    residual_ref,
    ffn_ref,
    kv_all,
    acc_ref,
    total_ref,
    token_rows,
    wo,
    dy_send,
    dy_recv,
    kv_send,
    kv_recv,
    swap_send,
    swap_recv,
    wo_send,
    wo_recv,
    window_send,
    window_recv,
    out_sem,
):
    outer, inner, fsdp = here = place()
    me = member_of(here)
    lane = lane_of(here)
    part = x_ref.shape[1]
    half = kv_ref.shape[0] // 2
    sub = half // 2
    wide = 2 * sub
    width = x_ref.shape[2]
    depth = width // 2
    reach = gate_far.shape[1]
    tiles = 2 * (reach // BLOCK) - 1
    their = lane_of(chip_peer(1))
    start = (their // 2 * tiles + their % 2 * (reach // BLOCK - 1)) * BLOCK
    window = pl.ds(pl.multiple_of(start, BLOCK), reach)
    rows = depth // 4

    def outer_peer(k):
        return ((outer + k) % steps, inner, fsdp)

    def window_copy(n):
        src, dst = ((gate_any, gate_far), (up_any, up_far))[n // 4]
        at = pl.ds(n % 4 * rows, rows)
        return remote(
            src.at[at, window], dst.at[at], window_send.at[n], window_recv.at[n], chip_peer(1)
        )

    ready = greet(
        [outer_peer(k) for k in range(1, steps)] + [group_peer(k) for k in range(1, 8)]
    )
    mine_at = pl.ds(pl.multiple_of(fsdp * depth, depth), depth)
    far_at = pl.ds(pl.multiple_of((1 - fsdp) * depth, depth), depth)
    wo_load = pltpu.make_async_copy(wo_any, wo.at[mine_at], out_sem.at[2])
    wo_load.start()
    own_dy = pltpu.make_async_copy(dy_ref, cot_out.at[slot_of(here)], out_sem.at[0])
    own_dy.start()
    kv_all[outer] = kv_ref[...]
    acc_ref[...] = jnp.zeros_like(acc_ref)
    total_ref[...] = jnp.zeros_like(total_ref)
    ready()

    def kv_copy(slot, late, source):
        at = pl.ds(late * half, half)
        return remote(
            kv_ref.at[at],
            kv_all.at[source, at],
            kv_send.at[late, slot],
            kv_recv.at[late, source],
            (slot, inner, fsdp),
        )

    @pl.loop(1, steps)
    def _(k):
        slot = (outer + steps - k) % steps
        kv_copy(slot, 0, outer).start()

        @pl.when(slot < outer)
        def _():
            kv_copy(slot, 1, outer).start()

    share = Exchange(wo_any, wo_far, wo_far, wo_send, wo_recv)
    share.start()
    cot = Gather(
        [dy_ref.at[n] for n in range(2)],
        lambda device: [cot_out.at[slot_of(device), n] for n in range(2)],
        dy_send,
        dy_recv,
    )
    cot.start()
    for n in range(4):
        window_copy(n).start()

    def block(slot, row, size, col, mask):
        kv = kv_all[slot, pl.ds(pl.multiple_of(row, sub), size), :]
        cols = pl.ds(pl.multiple_of(col, wide), wide)
        probs = jnp.exp2(dot(kv, qt_ref[:, cols]) * SCORE2)
        if mask is not None:
            probs = jnp.where(mask, probs, 0.0)
        total_ref[:, cols] += jnp.sum(probs.reshape(size // 8, 8, wide), axis=0)
        acc_ref[:, cols] += dot(kv, probs.astype(BF16), ((0,), (0,)))

    key = lax.broadcasted_iota(jnp.int32, (sub, wide), 0)
    query = lax.broadcasted_iota(jnp.int32, (sub, wide), 1) % sub
    diagonal = key <= query

    @pl.loop(0, 2)
    def _(late):
        block(outer, late * half, sub, late * 2 * wide, diagonal)
        block(outer, late * half, sub, late * 2 * wide + wide, None)
        block(outer, late * half + sub, sub, late * 2 * wide + wide, diagonal)

    @pl.loop(0, 2)
    def _(n):
        block(outer, 0, half, (2 + n) * wide, None)

    share.share()
    cot.pass_on(1)

    @pl.loop(1, steps)
    def _(k):
        slot = (outer + k) % steps
        late = jnp.where(slot < outer, 0, 1)
        kv_copy(slot, 0, slot).wait_recv()

        @pl.when(slot > outer)
        def _():
            kv_copy(slot, 1, slot).wait_recv()

        @pl.loop(0, 2)
        def _(n):
            block(slot, 0, half, (2 + n) * wide, None)
            block(slot, late * half, half, (late * 2 + n) * wide, None)

    @pl.loop(0, 4)
    def _(tile):
        heads = []
        for head in range(2):
            cols = pl.ds(pl.multiple_of(tile * wide + head * sub, sub), sub)
            total = jnp.sum(total_ref[:, cols], axis=0, keepdims=True)
            values = acc_ref[HEAD:, cols] / total
            attn_t_ref[:, cols] = values
            log_ref[:, cols] = jnp.log2(total)
            heads.append(values)
        inside = pl.ds(pl.multiple_of((tile % 2) * sub, sub), sub)
        attn_ref[tile // 2, inside, :] = jnp.concatenate(heads, axis=0).T.astype(BF16)

    def landing(device):
        cols = pl.ds(pl.multiple_of(lane_of(device) * 2 * HEAD, 2 * HEAD), 2 * HEAD)
        return [token_rows.at[n, :, cols] for n in range(2)]

    def swap_copy(k, n, owner):
        device = group_peer(k)
        return remote(
            token_at(attn_ref, device, part)[n],
            landing(owner)[n],
            swap_send.at[n, k],
            swap_recv.at[n, slot_of(owner)],
            device,
        )

    for k in range(1, 8):
        for n in range(2):
            swap_copy(k, n, here).start()
    for n in range(4, 8):
        window_copy(n).start()
    own_cols = pl.ds(pl.multiple_of(lane * 2 * HEAD, 2 * HEAD), 2 * HEAD)
    token_rows[0, :, own_cols] = attn_ref[0, pl.ds(early_row(me, part), part), :]
    token_rows[1, :, own_cols] = attn_ref[1, pl.ds(late_row(me, part), part), :]
    @pl.loop(1, steps)
    def _(k):
        slot = (outer + k) % steps

        @pl.when(slot < outer)
        def _():
            kv_all[slot, pl.ds(half, half), :] = jnp.zeros((half, 2 * HEAD), BF16)

    kv_store = pltpu.make_async_copy(kv_all, kv_out, out_sem.at[1])
    kv_store.start()
    share.finish()
    far_load = pltpu.make_async_copy(wo_far, wo.at[far_at], out_sem.at[3])
    far_load.start()
    cot.pass_on(2)
    cot.pass_on(3)
    wo_load.wait()
    far_load.wait()
    for k in range(1, 8):
        for n in range(2):
            swap_copy(k, n, group_peer(k)).wait_recv()
    for n in range(2):
        values = dot(token_rows[n], wo[...]) + x_ref[n].astype(F32)
        residual_ref[n] = values
        ffn_ref[n] = rms_rows(values, gain_ref[...]).astype(BF16)

    cot.finish()
    cot.drain()
    for k in range(1, 8):
        for n in range(2):
            swap_copy(k, n, here).wait_send()

    @pl.loop(1, steps)
    def _(k):
        slot = (outer + k) % steps
        kv_copy(slot, 0, outer).wait_send()

        @pl.when(slot < outer)
        def _():
            kv_copy(slot, 1, outer).wait_send()

    for n in range(8):
        window_copy(n).wait_recv()
        window_copy(n).wait_send()
    own_dy.wait()
    kv_store.wait()


SMEM = pl.BlockSpec(memory_space=pltpu.SMEM)
VMEM = pl.BlockSpec(memory_space=pltpu.VMEM)
ANY = pl.BlockSpec(memory_space=pl.ANY)
DMA = pltpu.SemaphoreType.DMA


def params(collective):
    return pltpu.CompilerParams(
        collective_id=collective, has_side_effects=True, vmem_limit_bytes=60 << 20
    )


def shape(dims, dtype=BF16):
    return jax.ShapeDtypeStruct(tuple(dims), dtype)


def front(x, gain, wq, wk, wv, freq, q_gain, k_gain, steps):
    part, width = x.shape[1:]
    half = 8 * part
    tokens = 2 * half
    depth = wq.shape[0]
    wide = 2 * HEAD
    window = pltpu.VMEM((depth, 2 * wide), BF16)
    return pl.pallas_call(
        functools.partial(front_kernel, steps),
        out_shape=(
            shape((2, half, width)),
            shape((tokens, 2 * wide), F32),
            shape((2 * tokens, wide)),
            shape((wide, 2 * tokens)),
            shape((tokens, wide)),
            shape((tokens, wide), F32),
            shape((tokens, wide), F32),
        ),
        in_specs=[VMEM] * 2 + [ANY] * 3 + [VMEM] * 3,
        out_specs=[ANY] + [VMEM] * 6,
        scratch_shapes=[
            pltpu.VMEM((2, part, width), BF16),
            pltpu.VMEM((2, half, width), BF16),
            pltpu.VMEM((2, 2, depth, wide), BF16),
            window,
            window,
            window,
            DMA((2, 8)),
            DMA((2, 8)),
            DMA((2, 3)),
            DMA((2,)),
            DMA,
        ],
        compiler_params=params(0),
        name="front",
    )(x, gain, wq, wk, wv, freq, q_gain, k_gain)


def middle(x, dy, qt, kv, gain, wo, gate, up, reach, steps):
    part, width = x.shape[1:]
    tokens = kv.shape[0]
    half = tokens // 2
    depth = wo.shape[0]
    return pl.pallas_call(
        functools.partial(middle_kernel, steps),
        out_shape=(
            shape((steps, tokens, 2 * HEAD)),
            shape((8, 2, part, width)),
            shape((depth, width)),
            shape((depth, reach)),
            shape((depth, reach)),
            shape((HEAD, 2 * tokens), F32),
            shape((1, 2 * tokens), F32),
            shape((2, half, 2 * HEAD)),
            shape((2, part, width), F32),
            shape((2, part, width)),
        ),
        in_specs=[VMEM] * 5 + [ANY] * 3,
        out_specs=[ANY] * 5 + [VMEM] * 5,
        scratch_shapes=[
            pltpu.VMEM((steps, tokens, 2 * HEAD), BF16),
            pltpu.VMEM((2 * HEAD, 2 * tokens), F32),
            pltpu.VMEM((8, 2 * tokens), F32),
            pltpu.VMEM((2, part, width), BF16),
            pltpu.VMEM((width, width), BF16),
            DMA((2, 8)),
            DMA((2, 8)),
            DMA((2, steps)),
            DMA((2, steps)),
            DMA((2, 8)),
            DMA((2, 8)),
            DMA((4,)),
            DMA((4,)),
            DMA((8,)),
            DMA((8,)),
            DMA((4,)),
        ],
        compiler_params=params(1),
        name="middle",
    )(x, dy, qt, kv, gain, wo, gate, up)


def ffn_kernel(
    steps,
    ffn_ref,
    residual_ref,
    dy_ref,
    gain_ref,
    cot_any,
    gate_any,
    gate_far,
    up_any,
    up_far,
    down_any,
    wo_any,
    wo_far,
    out_ref,
    d_res_ref,
    grad_ref,
    d_gain_ref,
    d_gate_ref,
    d_up_ref,
    down_ref,
    gate,
    up,
    down,
    wo,
    cot,
    land,
    d_hidden,
    hidden,
    d_gate,
    d_up,
    keep,
    near_send,
    near_land,
    sum_send,
    sum_land,
    d_down,
    down_send,
    down_land,
    swap_own,
    load_sem,
    ffn_send,
    ffn_recv,
    near_ssem,
    near_rsem,
    sum_ssem,
    sum_rsem,
    down_ssem,
    down_rsem,
    swap_send,
    swap_recv,
):
    outer, inner, fsdp = here = place()
    part, width = ffn_ref.shape[1:]
    depth = width // 2
    rows = 2 * part
    pair = 2 * rows
    reach = gate.shape[1]
    odd = inner % 2
    my_slot = slot_of(here)
    me = member_of(here)
    lane = lane_of(here)
    tiles = 2 * (reach // BLOCK) - 1
    step = (reach // BLOCK - 1) * BLOCK
    start = pl.multiple_of((lane // 2) * tiles * BLOCK + odd * step, BLOCK)
    down_start = pl.multiple_of((inner // 2) * tiles * BLOCK + odd * step, BLOCK)
    mine_at = pl.ds(pl.multiple_of(fsdp * depth, depth), depth)
    far_at = pl.ds(pl.multiple_of((1 - fsdp) * depth, depth), depth)
    pad = BLOCK // 2

    def outer_peer(k):
        return ((outer + k) % steps, inner, fsdp)

    ready = greet(
        [outer_peer(k) for k in range(1, steps)] + [group_peer(k) for k in range(1, 8)]
    )
    loads = [
        pltpu.make_async_copy(src, dst, load_sem.at[n])
        for n, (src, dst) in enumerate(
            (
                (down_any.at[pl.ds(down_start, reach)], down),
                (cot_any, cot),
                (gate_any.at[:, pl.ds(start, reach)], gate.at[mine_at]),
                (gate_far, gate.at[far_at]),
                (up_any.at[:, pl.ds(start, reach)], up.at[mine_at]),
                (up_far, up.at[far_at]),
                (wo_any, wo.at[mine_at]),
                (wo_far, wo.at[far_at]),
            )
        )
    ]
    for copy in loads:
        copy.start()
    ready()
    gather = Gather(
        [ffn_ref],
        lambda device: [land.at[pl.ds(pl.multiple_of(slot_of(device) * 2, 2), 2)]],
        ffn_send,
        ffn_recv,
    )
    gather.start()
    land[pl.ds(pl.multiple_of(my_slot * 2, 2), 2)] = ffn_ref[...]
    loads[0].wait()
    loads[1].wait()

    def chip_at(n):
        return slot_of(chip_peer(n)) // 2

    def chip_rows(n):
        return pl.ds(pl.multiple_of(chip_at(n) * pair, pair), pair)

    def four(n):
        return pl.ds(pl.multiple_of(chip_at(n) * 4, 4), 4)

    @pl.loop(0, 4)
    def _(n):
        values = cot[four(n)].reshape(pair, width)
        d_hidden[chip_rows(n), :] = dot(values, down[...], ((1,), (1,)))

    for copy in loads[2:6]:
        copy.wait()
    col = lax.broadcasted_iota(jnp.int32, (pair, reach), 1)
    valid = (col >= odd * pad) & (col < reach - pad + odd * pad)

    def near_copy(n):
        return remote(
            near_send.at[n], near_land.at[n], near_ssem.at[n], near_rsem.at[n], sibling()
        )

    def sum_copy(n):
        return remote(
            sum_send.at[n], sum_land.at[n], sum_ssem.at[n], sum_rsem.at[n], chip_peer(n)
        )

    def add_up(n):
        near_copy(n).wait_recv()
        total = keep[n] + near_land[n].astype(F32)

        @pl.when(n == 0)
        def _():
            keep[0] = total

        @pl.when(n > 0)
        def _():
            sum_send[n] = total.astype(BF16)
            sum_copy(n).start()

    @pl.loop(0, 4)
    def _(n):
        @pl.when(n > 0)
        def _():
            gather.pass_on(n)

        gather.wait(chip_peer(n, 1))
        at = chip_rows(n)
        values = land[four(n)].reshape(pair, width)
        gate_pre = dot(values, gate[...])
        up_pre = dot(values, up[...])
        sigmoid = jax.nn.sigmoid(gate_pre)
        silu = gate_pre * sigmoid
        hidden[at, :] = jnp.where(valid, silu * up_pre, 0.0).astype(BF16)
        back = jnp.where(valid, d_hidden[at, :], 0.0)
        d_gate[at, :] = (back * up_pre * sigmoid * (1.0 + gate_pre * (1.0 - sigmoid))).astype(BF16)
        d_up[at, :] = (back * silu).astype(BF16)
        for core in range(2):
            some = pl.ds(pl.multiple_of(chip_at(n) * pair + core * rows, rows), rows)
            total = dot(d_gate[some, :], gate[...], ((1,), (1,)))
            total = total + dot(d_up[some, :], up[...], ((1,), (1,)))

            @pl.when(odd == core)
            def _():
                keep[n] = total

            @pl.when(odd != core)
            def _():
                near_send[n] = total.astype(BF16)

        near_copy(n).start()

        @pl.when(n > 0)
        def _():
            add_up(n - 1)

    cot_rows = cot.reshape(8 * rows, width)
    land_rows = land.reshape(8 * rows, width)

    @pl.loop(0, reach // BLOCK)
    def _(tile):
        at = pl.ds(pl.multiple_of(tile * BLOCK, BLOCK), BLOCK)
        d_down[at, :] = dot(hidden[:, at], cot_rows[...], ((0,), (0,)))

    add_up(3)
    down_per = down_send.shape[1]
    for z in range(steps):
        at = z * down_per
        even_rows = d_down[at : at + down_per, :]
        odd_rows = d_down[at + pad : at + pad + down_per, :]
        down_send[z] = jnp.where(odd > 0, odd_rows, even_rows).astype(BF16)

    def down_copy(slot, source):
        return remote(
            down_send.at[slot],
            down_land.at[source],
            down_ssem.at[slot],
            down_rsem.at[source],
            (slot, inner, fsdp),
        )

    @pl.loop(1, steps)
    def _(k):
        down_copy((outer + k) % steps, outer).start()

    @pl.loop(0, 4)
    def _(n):
        total = dot(hidden[chip_rows(n), :], down[...])
        slots = pl.ds(pl.multiple_of(chip_at(n) * 2, 2), 2)
        out_ref[slots] = total.reshape(2, rows, width).astype(BF16)

    for copy in loads[6:]:
        copy.wait()
    error = keep[0]
    for n in (1, 2, 3):
        sum_copy(n).wait_recv()
        error = error + sum_land[n].astype(F32)
    residual = residual_ref[...].reshape(rows, width)
    inverse = lax.rsqrt(jnp.mean(residual * residual, axis=-1, keepdims=True) + EPS)
    scaled = error * gain_ref[...]
    inner_mean = jnp.mean(scaled * residual, axis=-1, keepdims=True)
    back = inverse * scaled - residual * (inverse * inverse * inverse) * inner_mean
    d_gain_ref[...] = jnp.sum(error * residual * inverse, axis=0, keepdims=True)
    d_residual = dy_ref[...].reshape(rows, width).astype(F32) + back
    d_res_ref[...] = d_residual.reshape(2, part, width)
    attn_grad = dot(d_residual.astype(BF16), wo[...], ((1,), (1,)))
    swap_own[...] = attn_grad.astype(BF16).reshape(2, part, width)

    def head_cols(device):
        return pl.ds(pl.multiple_of(lane_of(device) * 2 * HEAD, 2 * HEAD), 2 * HEAD)

    def swap_copy(k, n, owner):
        device = group_peer(k)
        return remote(
            swap_own.at[n, :, head_cols(device)],
            token_at(grad_ref, owner, part)[n],
            swap_send.at[n, k],
            swap_recv.at[n, slot_of(owner)],
            device,
        )

    for k in range(1, 8):
        for n in range(2):
            swap_copy(k, n, here).start()
    grad_ref[0, pl.ds(early_row(me, part), part)] = swap_own[0, :, head_cols(here)]
    grad_ref[1, pl.ds(late_row(me, part), part)] = swap_own[1, :, head_cols(here)]

    per = d_gate_ref.shape[1]
    many = BLOCK // per

    @pl.loop(0, width // BLOCK)
    def _(tile):
        at = pl.ds(pl.multiple_of(tile * BLOCK, BLOCK), BLOCK)
        for right, ref in ((d_gate, d_gate_ref), (d_up, d_up_ref)):
            value = dot(land_rows[:, at], right[...], ((0,), (0,)))
            ref[pl.ds(tile * many, many)] = value.reshape(many, per, reach).astype(BF16)

    down_total = down_send[outer].astype(F32)
    for k in range(1, steps):
        source = (outer + k) % steps
        down_copy(source, source).wait_recv()
        down_total = down_total + down_land[source].astype(F32)
    down_ref[...] = down_total.astype(BF16)

    for k in range(1, 8):
        for n in range(2):
            swap_copy(k, n, group_peer(k)).wait_recv()
            swap_copy(k, n, here).wait_send()
    for n in range(4):
        near_copy(n).wait_send()
        if n:
            sum_copy(n).wait_send()
    for k in range(1, steps):
        down_copy((outer + k) % steps, outer).wait_send()
    gather.drain()


def ffn(ffn_rows, residual, dy, gain, cot, weights, steps):
    part, width = ffn_rows.shape[1:]
    reach = weights[1].shape[1]
    own_ff = reach - BLOCK // 2
    rows = 2 * part
    half = 8 * part
    tokens = 2 * half
    devices = 8 * steps
    slices = pltpu.VMEM((steps, own_ff // steps, width), BF16)
    some = pltpu.VMEM((4, rows, width), BF16)
    return pl.pallas_call(
        functools.partial(ffn_kernel, steps),
        out_shape=(
            shape((8, rows, width)),
            shape((2, part, width), F32),
            shape((2, half, 2 * HEAD)),
            shape((1, width), F32),
            shape((devices, width // devices, reach)),
            shape((devices, width // devices, reach)),
            shape((own_ff // steps, width)),
        ),
        in_specs=[VMEM] * 4 + [ANY] * 8,
        out_specs=[VMEM] * 7,
        scratch_shapes=[
            pltpu.VMEM((width, reach), BF16),
            pltpu.VMEM((width, reach), BF16),
            pltpu.VMEM((reach, width), BF16),
            pltpu.VMEM((width, width), BF16),
            pltpu.VMEM((16, part, width), BF16),
            pltpu.VMEM((16, part, width), BF16),
            pltpu.VMEM((tokens, reach), F32),
            pltpu.VMEM((tokens, reach), BF16),
            pltpu.VMEM((tokens, reach), BF16),
            pltpu.VMEM((tokens, reach), BF16),
            pltpu.VMEM((4, rows, width), F32),
            some,
            some,
            some,
            some,
            pltpu.VMEM((reach, width), F32),
            slices,
            slices,
            pltpu.VMEM((2, part, width), BF16),
            DMA((8,)),
            DMA((1, 8)),
            DMA((1, 8)),
            DMA((4,)),
            DMA((4,)),
            DMA((4,)),
            DMA((4,)),
            DMA((steps,)),
            DMA((steps,)),
            DMA((2, 8)),
            DMA((2, 8)),
        ],
        compiler_params=params(2),
        name="ffn",
    )(ffn_rows, residual, dy, gain, cot, *weights)


def back_kernel(
    steps,
    qt_ref,
    q_ref,
    grad_ref,
    attn_t_ref,
    log_ref,
    kv_ref,
    proj_ref,
    cos_ref,
    sin_ref,
    qg_ref,
    kg_ref,
    x_ref,
    d_res_ref,
    residual_ref,
    attn_ref,
    gain_ref,
    ffn_gain_ref,
    normed_any,
    wq_any,
    wk_any,
    wv_any,
    d_gate_any,
    d_up_any,
    d_down_any,
    out_any,
    block_ref,
    dx_ref,
    gains_ref,
    own_q_ref,
    own_k_ref,
    own_v_ref,
    own_o_ref,
    own_gate_ref,
    own_up_ref,
    own_down_ref,
    normed,
    wq,
    wk,
    wv,
    gt_ref,
    g_ref,
    delta_ref,
    acc_ref,
    dkv_ref,
    dkv_send,
    dkv_land,
    d_qkv,
    tokens_land,
    dq_rows,
    dk_rows,
    dv_rows,
    d_weights,
    d_wo,
    res_own,
    res_land,
    out_land,
    gate_land,
    up_land,
    qkv_land,
    down_land,
    wo_land,
    sums,
    sums_land,
    load_sem,
    gate_send,
    gate_recv,
    up_send,
    up_recv,
    qkv_send,
    qkv_recv,
    down_sem,
    wo_send,
    wo_recv,
    out_send,
    out_recv,
    res_send,
    res_recv,
    share_send,
    share_recv,
    kv_send,
    kv_recv,
    swap_send,
    swap_recv,
    near_send,
    near_recv,
    far_send,
    far_recv,
):
    outer, inner, fsdp = here = place()
    lane = lane_of(here)
    number = number_of(here)
    me = member_of(here)
    my_slot = slot_of(here)
    count = steps * 8
    part, width = x_ref.shape[1:]
    rows = 2 * part
    half = normed.shape[1]
    sub = half // 2
    wide = 2 * sub
    depth = width // 2
    twice = 2 * HEAD

    barrier = pltpu.get_barrier_semaphore()

    @pl.loop(1, count)
    def _(k):
        pl.semaphore_signal(
            barrier,
            inc=1,
            device_id=member_device((number + k) % count),
            device_id_type=pl.DeviceIdType.MESH,
        )

    mine_at = pl.ds(pl.multiple_of(fsdp * depth, depth), depth)
    far_at = pl.ds(pl.multiple_of((1 - fsdp) * depth, depth), depth)
    loads = [
        pltpu.make_async_copy(src, dst, load_sem.at[n])
        for n, (src, dst) in enumerate(
            (
                (normed_any, normed),
                (wq_any, wq.at[mine_at]),
                (wk_any, wk.at[mine_at]),
                (wv_any, wv.at[mine_at]),
            )
        )
    ]
    for copy in loads:
        copy.start()
    res_own[...] = d_res_ref[...].astype(BF16)
    acc_ref[...] = jnp.zeros_like(acc_ref)
    dkv_ref[...] = jnp.zeros_like(dkv_ref)
    low = lax.broadcasted_iota(jnp.int32, (sub, twice), 1) < HEAD
    front = lax.broadcasted_iota(jnp.int32, (sub, twice), 1) % HEAD < HEAD // 2

    @pl.loop(0, 4)
    def _(tile):
        inside = pl.ds(pl.multiple_of((tile % 2) * sub, sub), sub)
        values = grad_ref[tile // 2, inside, :].astype(F32)
        flipped = pltpu.roll(values, HEAD, 1)
        for head, shifted in enumerate((flipped, values)):
            cols = pl.ds(pl.multiple_of(tile * wide + head * sub, sub), sub)
            shifted = jnp.where(low, 0.0, shifted)
            turned = shifted.T
            g_ref[cols, :] = shifted.astype(BF16)
            gt_ref[:, cols] = turned.astype(BF16)
            delta_ref[:, cols] = jnp.sum(
                turned[HEAD:] * attn_t_ref[:, cols], axis=0, keepdims=True
            )

    pl.semaphore_wait(barrier, count - 1)

    def rows_copy(src, land, ssem, rsem, target, source):
        key = lane_of(source) * steps + source[0]
        owner = number_of(target)
        return remote(src.at[owner], land.at[key], ssem.at[owner], rsem.at[key], target)

    def outer_peer(k):
        return ((outer + k) % steps, inner, fsdp)

    def send_rows(first, last, *refs):
        @pl.loop(first, last)
        def _(k):
            target = member_device((number + k) % count)
            for group in refs:
                rows_copy(*group, target, here).start()

    gate_refs = (d_gate_any, gate_land, gate_send, gate_recv)
    up_refs = (d_up_any, up_land, up_send, up_recv)
    qkv_refs = (d_weights, qkv_land, qkv_send, qkv_recv)

    down_number = lane * steps + outer
    down_out = remote(
        d_down_any, down_land, down_sem.at[0], down_sem.at[1], member_device(down_number)
    )
    down_away = down_number != number
    down_stay = pltpu.make_async_copy(d_down_any, down_land, down_sem.at[2])

    shares = [
        Exchange(src, ref.at[far_at], ref.at[mine_at], share_send.at[n], share_recv.at[n])
        for n, (src, ref) in enumerate(((wq_any, wq), (wk_any, wk), (wv_any, wv)))
    ]

    def out_copy(device, source):
        return remote(
            out_any.at[slot_of(device)],
            out_land.at[slot_of(source)],
            out_send.at[slot_of(device)],
            out_recv.at[slot_of(source)],
            device,
        )

    spread = Gather(
        [res_own.at[0], res_own.at[1]],
        lambda device: token_at(res_land, device, part),
        res_send,
        res_recv,
    )

    @pl.when(down_away)
    def _():
        down_out.start()

    @pl.when(jnp.logical_not(down_away))
    def _():
        down_stay.start()

    for share in shares:
        share.start()
    spread.start()
    res_land[0, pl.ds(early_row(me, part), part)] = res_own[0]
    res_land[1, pl.ds(late_row(me, part), part)] = res_own[1]
    own_out = pltpu.make_async_copy(out_any.at[my_slot], out_land.at[my_slot], load_sem.at[6])
    own_out.start()
    send_rows(1, count // 2, gate_refs)

    def block(slot, row, size, col, mask):
        at = pl.ds(pl.multiple_of(row, sub), size)
        kv = kv_ref[slot, at, :]
        cols = pl.ds(pl.multiple_of(col, wide), wide)
        probs = jnp.exp2(dot(kv, qt_ref[:, cols]) * SCORE2 - log_ref[:, cols])
        if mask is not None:
            probs = jnp.where(mask, probs, 0.0)
        grads = dot(kv, gt_ref[:, cols])
        grads = (probs * (grads - delta_ref[:, cols]) * SCORE).astype(BF16)
        dkv_ref[slot, at, :] += dot(grads, q_ref[cols, :]) + dot(
            probs.astype(BF16), g_ref[cols, :]
        )
        acc_ref[:, cols] += dot(kv, grads, ((0,), (0,)))

    def kv_copy(slot, late, source):
        at = pl.ds(late * half, half)
        return remote(
            dkv_send.at[slot, at],
            dkv_land.at[source, at],
            kv_send.at[late, slot],
            kv_recv.at[late, source],
            (slot, inner, fsdp),
        )

    @pl.loop(1, steps)
    def _(k):
        slot = (outer + k) % steps
        late = jnp.where(slot < outer, 0, 1)

        @pl.loop(0, 2)
        def _(n):
            block(slot, 0, half, (2 + n) * wide, None)
            block(slot, late * half, half, (late * 2 + n) * wide, None)

        dkv_send[slot] = dkv_ref[slot].astype(BF16)
        kv_copy(slot, 0, outer).start()

        @pl.when(slot > outer)
        def _():
            kv_copy(slot, 1, outer).start()

    for k in range(1, 8):
        out_copy(group_peer(k), here).start()
    spread.pass_on(1)
    for share in shares:
        share.share()
    key = lax.broadcasted_iota(jnp.int32, (sub, wide), 0)
    query = lax.broadcasted_iota(jnp.int32, (sub, wide), 1) % sub
    diagonal = key <= query

    @pl.loop(0, 2)
    def _(late):
        block(outer, late * half, sub, late * 2 * wide, diagonal)
        block(outer, late * half, sub, late * 2 * wide + wide, None)
        block(outer, late * half + sub, sub, late * 2 * wide + wide, diagonal)

    @pl.loop(0, 2)
    def _(n):
        block(outer, 0, half, (2 + n) * wide, None)

    def rope_back(grads, at):
        return grads * cos_ref[at, :] + halves(grads * sin_ref[at, :], front)

    def norm_back(raw, grads, gain):
        inverse = head_inverse(raw, low)
        scaled = grads * gain
        product = scaled * raw
        first = jnp.sum(jnp.where(low, product, 0.0), axis=-1, keepdims=True)
        second = jnp.sum(jnp.where(low, 0.0, product), axis=-1, keepdims=True)
        inner_mean = jnp.where(low, first, second) * (1.0 / HEAD)
        back = inverse * scaled - raw * (inverse * inverse * inverse) * inner_mean
        return back, jnp.sum(grads * raw * inverse, axis=0, keepdims=True)

    sums[...] = jnp.zeros_like(sums)

    @pl.loop(0, 4)
    def _(tile):
        heads = []
        for head in range(2):
            cols = pl.ds(pl.multiple_of(tile * wide + head * sub, sub), sub)
            heads.append(acc_ref[:HEAD, cols])
        at = pl.ds(pl.multiple_of(tile * sub, sub), sub)
        inside = pl.ds(pl.multiple_of((tile % 2) * sub, sub), sub)
        grads = rope_back(jnp.concatenate(heads, axis=0).T, at)
        back, gain = norm_back(proj_ref[at, :twice], grads, qg_ref[...])
        d_qkv[tile // 2, inside, :twice] = back.astype(BF16)
        sums[2:3, :twice] += gain

    @pl.loop(1, steps)
    def _(k):
        source = (outer + k) % steps
        kv_copy(source, 0, source).wait_recv()
        early = pl.ds(0, half)
        dkv_ref[outer, early, :] += dkv_land[source, early, :].astype(F32)

        @pl.when(source < outer)
        def _():
            kv_copy(source, 1, source).wait_recv()
            at = pl.ds(half, half)
            dkv_ref[outer, at, :] += dkv_land[source, at, :].astype(F32)

    @pl.loop(0, 4)
    def _(tile):
        at = pl.ds(pl.multiple_of(tile * sub, sub), sub)
        inside = pl.ds(pl.multiple_of((tile % 2) * sub, sub), sub)
        grads = dkv_ref[outer, at, :]
        raw = proj_ref[at, twice:]
        back, gain = norm_back(raw, jnp.where(low, rope_back(grads, at), 0.0), kg_ref[...])
        d_qkv[tile // 2, inside, twice:] = jnp.where(low, back, grads).astype(BF16)
        sums[2:3, twice : 2 * twice] += gain

    def lane_cols(device):
        return pl.ds(pl.multiple_of(lane_of(device) * 2 * twice, 2 * twice), 2 * twice)

    def swap_copy(k, n, owner):
        device = group_peer(k)
        return remote(
            token_at(d_qkv, device, part)[n],
            tokens_land.at[n, :, lane_cols(owner)],
            swap_send.at[n, k],
            swap_recv.at[n, slot_of(owner)],
            device,
        )

    for k in range(1, 8):
        for n in range(2):
            swap_copy(k, n, here).start()
    tokens_land[0, :, lane_cols(here)] = d_qkv[0, pl.ds(early_row(me, part), part), :]
    tokens_land[1, :, lane_cols(here)] = d_qkv[1, pl.ds(late_row(me, part), part), :]
    send_rows(count // 2, count, gate_refs)

    loads[0].wait()
    per = d_weights.shape[1]
    normed_rows = normed.reshape(2 * half, width)
    d_rows = d_qkv.reshape(2 * half, 2 * twice)

    @pl.loop(0, width // BLOCK)
    def _(tile):
        at = pl.ds(pl.multiple_of(tile * BLOCK, BLOCK), BLOCK)
        value = dot(normed_rows[:, at], d_rows[...], ((0,), (0,)))
        many = BLOCK // per
        d_weights[pl.ds(tile * many, many)] = value.reshape(many, per, 2 * twice).astype(BF16)

    send_rows(1, count, qkv_refs, up_refs)
    own_key = lane * steps + outer
    qkv_land[own_key] = d_weights[number]
    own_rows = [
        pltpu.make_async_copy(src.at[number], land.at[own_key], load_sem.at[n])
        for n, (src, land) in ((4, (d_gate_any, gate_land)), (5, (d_up_any, up_land)))
    ]
    for copy in own_rows:
        copy.start()
    spread.pass_on(2)
    spread.pass_on(3)

    for copy in loads[1:]:
        copy.wait()
    for share in shares:
        share.finish()
    for k in range(1, 8):
        for n in range(2):
            swap_copy(k, n, group_peer(k)).wait_recv()
    lower = lax.broadcasted_iota(jnp.int32, (rows, twice), 1) < HEAD
    for m in range(4):
        kv_pair = []
        for n in range(2):
            base = (2 * m + n) * 2 * twice
            values = tokens_land[:, :, base : base + 2 * twice].reshape(rows, 2 * twice)
            dq_rows[:, (2 * m + n) * twice : (2 * m + n + 1) * twice] = values[:, :twice]
            kv_pair.append(values[:, twice:].astype(F32))
        first, second = kv_pair
        at = slice(m * twice, (m + 1) * twice)
        dk_rows[:, at] = jnp.where(lower, first, pltpu.roll(second, HEAD, 1)).astype(BF16)
        dv_rows[:, at] = jnp.where(lower, pltpu.roll(first, HEAD, 1), second).astype(BF16)
    error = dot(dq_rows[...], wq[...], ((1,), (1,)))
    error = error + dot(dk_rows[...], wk[...], ((1,), (1,)))
    error = error + dot(dv_rows[...], wv[...], ((1,), (1,)))
    inputs = x_ref[...].reshape(rows, width).astype(F32)
    inverse = lax.rsqrt(jnp.mean(inputs * inputs, axis=-1, keepdims=True) + EPS)
    scaled = error * gain_ref[...]
    inner_mean = jnp.mean(scaled * inputs, axis=-1, keepdims=True)
    back = inverse * scaled - inputs * (inverse * inverse * inverse) * inner_mean
    dx_ref[...] = (d_res_ref[...].reshape(rows, width) + back).reshape(2, part, width)
    sums[0:1, :] = jnp.sum(error * inputs * inverse, axis=0, keepdims=True)
    sums[1:2, :] = ffn_gain_ref[...]

    def near_copy(k, owner):
        return remote(
            sums,
            sums_land.at[slot_of(owner)],
            near_send.at[k],
            near_recv.at[slot_of(owner)],
            group_peer(k),
        )

    def far_copy(k, owner):
        return remote(
            gains_ref, sums_land.at[8 + owner], far_send.at[k], far_recv.at[owner], outer_peer(k)
        )

    for k in range(1, 8):
        near_copy(k, here).start()

    spread.finish()
    value = dot(
        attn_ref[...].reshape(2 * half, twice), res_land[...].reshape(2 * half, width), ((0,), (0,))
    )
    d_wo[...] = value.reshape(d_wo.shape).astype(BF16)

    def slice_copy(chunk, source):
        target = member_device(lane * steps + chunk)
        return remote(
            d_wo.at[chunk], wo_land.at[source], wo_send.at[chunk], wo_recv.at[source], target
        )

    @pl.loop(0, steps)
    def _(k):
        chunk = (outer + k) % steps
        pl.when(lane * steps + chunk != number)(slice_copy(chunk, outer).start)

    @pl.when(number // steps == lane)
    def _():
        wo_land[outer] = d_wo[number % steps]

    own_out.wait()
    total = residual_ref[...].reshape(rows, width) + out_land[my_slot].astype(F32)
    for k in range(1, 8):
        device = group_peer(k)
        out_copy(device, device).wait_recv()
        total = total + out_land[slot_of(device)].astype(F32)
    block_ref[...] = total.reshape(2, part, width).astype(BF16)

    total = sums[...]
    for k in range(1, 8):
        near_copy(k, group_peer(k)).wait_recv()
        total = total + sums_land[slot_of(group_peer(k))]
    gains_ref[...] = total

    @pl.loop(1, steps)
    def _(k):
        far_copy(k, outer).start()

    for copy in own_rows:
        copy.wait()

    @pl.loop(1, count)
    def _(k):
        source = member_device((number + k) % count)
        rows_copy(*gate_refs, here, source).wait_recv()

    def added(land, which):
        total = land[which * steps].astype(F32)
        for z in range(1, steps):
            total = total + land[which * steps + z].astype(F32)
        return total

    reach = gate_land.shape[2]
    tiles = 2 * (reach // BLOCK) - 1
    step = reach - BLOCK

    def join_windows(land, ref):
        for pair in range(4):
            base = pair * tiles * BLOCK
            first, second = added(land, 2 * pair), added(land, 2 * pair + 1)
            ref[:, base : base + step] = first[:, :step]
            ref[:, base + step : base + reach] = first[:, step:] + second[:, :BLOCK]
            ref[:, base + reach : base + tiles * BLOCK] = second[:, BLOCK:]

    join_windows(gate_land, own_gate_ref)

    @pl.when(down_away)
    def _():
        down_out.wait_send()
        down_out.wait_recv()

    @pl.when(jnp.logical_not(down_away))
    def _():
        down_stay.wait()

    own_down_ref[...] = down_land[...].astype(F32)

    @pl.loop(1, count)
    def _(k):
        source = member_device((number + k) % count)
        rows_copy(*qkv_refs, here, source).wait_recv()
        rows_copy(*up_refs, here, source).wait_recv()

    join_windows(up_land, own_up_ref)
    for pair in range(4):
        first, second = added(qkv_land, 2 * pair), added(qkv_land, 2 * pair + 1)
        own_q_ref[:, 2 * pair * twice : (2 * pair + 1) * twice] = first[:, :twice]
        own_q_ref[:, (2 * pair + 1) * twice : (2 * pair + 2) * twice] = second[:, :twice]
        first, second = first[:, twice:], second[:, twice:]
        lower = lax.broadcasted_iota(jnp.int32, first.shape, 1) < HEAD
        at = slice(pair * twice, (pair + 1) * twice)
        own_k_ref[:, at] = jnp.where(lower, first, pltpu.roll(second, HEAD, 1))
        own_v_ref[:, at] = jnp.where(lower, pltpu.roll(first, HEAD, 1), second)

    @pl.loop(0, steps)
    def _(z):
        source = (z, (number // steps) % 4, (number // steps) // 4)
        pl.when(number_of(source) != number)(slice_copy(0, z).wait_recv)

    own_o_ref[...] = jnp.zeros_like(own_o_ref)

    @pl.loop(0, steps)
    def _(z):
        own_o_ref[...] += wo_land[z].astype(F32)

    @pl.loop(1, steps)
    def _(k):
        far_copy(k, outer).wait_send()

    @pl.loop(1, steps)
    def _(k):
        source = (outer + k) % steps
        far_copy(k, source).wait_recv()
        gains_ref[...] += sums_land[8 + source]

    for k in range(1, 8):
        near_copy(k, here).wait_send()
        out_copy(group_peer(k), here).wait_send()
        for n in range(2):
            swap_copy(k, n, here).wait_send()
    spread.drain()

    @pl.loop(0, steps)
    def _(chunk):
        pl.when(lane * steps + chunk != number)(slice_copy(chunk, outer).wait_send)

    @pl.loop(1, steps)
    def _(k):
        slot = (outer + k) % steps
        kv_copy(slot, 0, outer).wait_send()

        @pl.when(slot > outer)
        def _():
            kv_copy(slot, 1, outer).wait_send()

    @pl.loop(1, count)
    def _(k):
        target = member_device((number + k) % count)
        for refs in (gate_refs, up_refs, qkv_refs):
            rows_copy(*refs, target, here).wait_send()


def back(args, steps):
    q_t, q_cols = args[0], args[1]
    kv, x = args[5], args[11]
    normed, wq, wk = args[17], args[18], args[19]
    d_gate, d_down = args[21], args[23]
    part, width = x.shape[1:]
    half = normed.shape[1]
    tokens = 2 * half
    rows = 2 * part
    count = steps * 8
    per = width // count
    reach = d_gate.shape[2]
    ff = (2 * (reach // BLOCK) - 1) * BLOCK * 4
    twice = 2 * HEAD
    q_cols_all, kv_cols = wq.shape[1], wk.shape[1]
    return pl.pallas_call(
        functools.partial(back_kernel, steps),
        out_shape=(
            shape((2, part, width)),
            shape((2, part, width), F32),
            shape((8, width), F32),
            shape((per, q_cols_all), F32),
            shape((per, kv_cols), F32),
            shape((per, kv_cols), F32),
            shape((twice // steps, width), F32),
            shape((per, ff), F32),
            shape((per, ff), F32),
            shape(d_down.shape, F32),
        ),
        in_specs=[VMEM] * 17 + [ANY] * 8,
        out_specs=[VMEM] * 10,
        scratch_shapes=[
            pltpu.VMEM(normed.shape, BF16),
            pltpu.VMEM((width, q_cols_all), BF16),
            pltpu.VMEM((width, kv_cols), BF16),
            pltpu.VMEM((width, kv_cols), BF16),
            pltpu.VMEM(q_t.shape, BF16),
            pltpu.VMEM(q_cols.shape, BF16),
            pltpu.VMEM((1, 2 * tokens), F32),
            pltpu.VMEM(q_t.shape, F32),
            pltpu.VMEM(kv.shape, F32),
            pltpu.VMEM(kv.shape, BF16),
            pltpu.VMEM(kv.shape, BF16),
            pltpu.VMEM((2, half, 2 * twice), BF16),
            pltpu.VMEM((2, part, 16 * twice), BF16),
            pltpu.VMEM((rows, q_cols_all), BF16),
            pltpu.VMEM((rows, kv_cols), BF16),
            pltpu.VMEM((rows, kv_cols), BF16),
            pltpu.VMEM((count, per, 2 * twice), BF16),
            pltpu.VMEM((steps, twice // steps, width), BF16),
            pltpu.VMEM((2, part, width), BF16),
            pltpu.VMEM((2, half, width), BF16),
            pltpu.VMEM((8, rows, width), BF16),
            pltpu.VMEM((count, per, reach), BF16),
            pltpu.VMEM((count, per, reach), BF16),
            pltpu.VMEM((count, per, 2 * twice), BF16),
            pltpu.VMEM(d_down.shape, BF16),
            pltpu.VMEM((steps, twice // steps, width), BF16),
            pltpu.VMEM((8, width), F32),
            pltpu.VMEM((8 + steps, 8, width), F32),
            DMA((7,)),
            DMA((count,)),
            DMA((count,)),
            DMA((count,)),
            DMA((count,)),
            DMA((count,)),
            DMA((count,)),
            DMA((3,)),
            DMA((steps,)),
            DMA((steps,)),
            DMA((8,)),
            DMA((8,)),
            DMA((2, 8)),
            DMA((2, 8)),
            DMA((3, 4)),
            DMA((3, 4)),
            DMA((2, steps)),
            DMA((2, steps)),
            DMA((2, 8)),
            DMA((2, 8)),
            DMA((8,)),
            DMA((8,)),
            DMA((steps,)),
            DMA((steps,)),
        ],
        compiler_params=params(3),
        name="back",
    )(*args)


def local(
    block_input, dy, attn_gain, q_gain, k_gain, ffn_gain, wq, wk, wv, wo, w_gate, w_up, w_down
):
    steps = lax.axis_size("outer")
    group = lax.axis_size("inner") * lax.axis_size("fsdp")
    part, width = block_input.shape[2:]
    tiles = 2 * w_gate.shape[1] // group // BLOCK
    reach = (tiles + 1) // 2 * BLOCK
    x = block_input.reshape(2, part, width)
    cot = dy.reshape(2, part, width)
    index = jnp.arange(2 * HEAD, dtype=jnp.int32) % (HEAD // 2)
    frequency = (ROPE_BASE ** (-2.0 * index.astype(F32) / HEAD))[None]
    q_gain2 = jnp.tile(q_gain, 2)[None]
    k_gain2 = jnp.tile(k_gain, 2)[None]
    normed, proj, q_cols, q_t, kv_own, cos, sin = front(
        x, attn_gain[None], wq, wk, wv, frequency, q_gain2, k_gain2, steps
    )
    kv, cot_group, wo_far, gate_far, up_far, attn_t, log_total, attn, residual, ffn_rows = middle(
        x, cot, q_t, kv_own, ffn_gain[None], wo, w_gate, w_up, reach, steps
    )
    partial, d_residual, attn_grad, d_ffn_gain, d_gate, d_up, d_down = ffn(
        ffn_rows,
        residual,
        cot,
        ffn_gain[None],
        cot_group.reshape(2 * group, part, width),
        (w_gate, gate_far, w_up, up_far, w_down, wo, wo_far),
        steps,
    )
    result, grad_in, gains, own_q, own_k, own_v, own_o, own_gate, own_up, own_down = back(
        (
            q_t,
            q_cols,
            attn_grad,
            attn_t,
            log_total,
            kv,
            proj,
            cos,
            sin,
            q_gain2,
            k_gain2,
            x,
            d_residual,
            residual,
            attn,
            attn_gain[None],
            d_ffn_gain,
            normed,
            wq,
            wk,
            wv,
            d_gate,
            d_up,
            d_down,
            partial,
        ),
        steps,
    )
    return (
        result.reshape(block_input.shape),
        grad_in.reshape(block_input.shape),
        gains[0],
        gains[2, :HEAD] + gains[2, HEAD : 2 * HEAD],
        gains[2, 2 * HEAD : 3 * HEAD],
        gains[1],
        own_q,
        own_k,
        own_v,
        own_o,
        own_gate,
        own_up,
        own_down,
    )


def solution(mesh):
    ctx, fsdp = mesh.shape["ctx"], mesh.shape["fsdp"]
    inner = 8 // fsdp
    grid = Mesh(mesh.devices.reshape(ctx // inner, inner, fsdp), EVERY)
    tokens = P(None, ("outer", "inner"), "fsdp", None)
    shard = P("fsdp", None)
    owned = P(EVERY, None)
    return jax.shard_map(
        local,
        mesh=grid,
        in_specs=(tokens, tokens) + (P(),) * 4 + (shard,) * 7,
        out_specs=(tokens, tokens) + (P(),) * 4 + (owned,) * 7,
        check_vma=False,
    )
```
